32 devices in a mesh: tp: 8 (over z, y), cp: 4 (over x, core).
Axes of the slice: x: 2, y: 2, z: 4, core: 2. Of those that a mesh axis runs over, the one named last changes fastest.
Arguments:
- hidden: bfloat16 [3, 4096, 2048], P(None, 'cp')
- grad_out: bfloat16 [3, 4096, 2048], P(None, 'cp')
- w_query: bfloat16 [2048, 8, 256], P(None, 'tp')
- w_key: bfloat16 [2048, 256], replicated
- w_value: bfloat16 [2048, 256], replicated
- w_out: bfloat16 [8, 256, 2048], P('tp')
Outputs:
- output 1: bfloat16 [3, 4096, 2048], P(None, 'cp')
- output 2: bfloat16 [3, 4096, 2048], P(None, 'cp')
- output 3: float32 [2048, 8, 256], P(None, 'tp')
- output 4: float32 [2048, 256], replicated
- output 5: float32 [2048, 256], replicated
- output 6: float32 [8, 256, 2048], P('tp')
All inputs are finite; a program needn't handle non-finite values.
Results may differ from the reference program's by a relative error of at most 0.010984.
Values are sent between devices in bfloat16 or wider.
A program may use at most 1 GiB of HBM per device.

```python
import jax
import jax.numpy as jnp
from jax import lax

BATCH = 3
SEQ = 4096
D_MODEL = 2048
HEADS = 8
HEAD_DIM = 256
Q_ROWS = 128


def rope_tables(positions):
    half_dim = HEAD_DIM // 2
    inv_freq = 1.0 / jnp.power(10000.0, jnp.arange(half_dim, dtype=jnp.float32) * (2.0 / HEAD_DIM))
    angles = positions.astype(jnp.float32)[:, None] * inv_freq[None, :]
    return jnp.cos(angles), jnp.sin(angles)


def rotate(rot_in, cos_tab, sin_tab):
    half_dim = rot_in.shape[-1] // 2
    low_half = rot_in[..., :half_dim]
    high_half = rot_in[..., half_dim:]
    return jnp.concatenate([low_half * cos_tab - high_half * sin_tab, high_half * cos_tab + low_half * sin_tab], axis=-1)


def unrotate(rot_in, cos_tab, sin_tab):
    half_dim = rot_in.shape[-1] // 2
    low_half = rot_in[..., :half_dim]
    high_half = rot_in[..., half_dim:]
    return jnp.concatenate([low_half * cos_tab + high_half * sin_tab, high_half * cos_tab - low_half * sin_tab], axis=-1)


def setup_inputs(seed: int = 0) -> dict:
    sub_keys = jax.random.split(jax.random.key(seed), 6)
    hidden = jax.random.normal(sub_keys[0], (BATCH, SEQ, D_MODEL), jnp.float32)
    grad_out = jax.random.normal(sub_keys[1], (BATCH, SEQ, D_MODEL), jnp.float32)
    in_scale = D_MODEL ** -0.5
    w_query = jax.random.normal(sub_keys[2], (D_MODEL, HEADS, HEAD_DIM), jnp.float32) * in_scale
    w_key = jax.random.normal(sub_keys[3], (D_MODEL, HEAD_DIM), jnp.float32) * in_scale
    w_value = jax.random.normal(sub_keys[4], (D_MODEL, HEAD_DIM), jnp.float32) * in_scale
    w_out = jax.random.normal(sub_keys[5], (HEADS, HEAD_DIM, D_MODEL), jnp.float32) * (HEADS * HEAD_DIM) ** -0.5
    return {"hidden": hidden.astype(jnp.bfloat16), "grad_out": grad_out.astype(jnp.bfloat16), "w_query": w_query.astype(jnp.bfloat16), "w_key": w_key.astype(jnp.bfloat16), "w_value": w_value.astype(jnp.bfloat16), "w_out": w_out.astype(jnp.bfloat16)}


def reference(hidden, grad_out, w_query, w_key, w_value, w_out):
    q_scale = HEAD_DIM ** -0.5
    n_blocks = SEQ // Q_ROWS
    cos_tab, sin_tab = rope_tables(jnp.arange(SEQ))
    flat_hidden = hidden.reshape(BATCH * SEQ, D_MODEL)
    key_pre = jnp.dot(flat_hidden, w_key, preferred_element_type=jnp.float32).reshape(BATCH, SEQ, HEAD_DIM)
    key_rot = rotate(key_pre, cos_tab, sin_tab).astype(jnp.bfloat16).astype(jnp.float32)
    val_all = jnp.dot(flat_hidden, w_value, preferred_element_type=jnp.float32).reshape(BATCH, SEQ, HEAD_DIM).astype(jnp.bfloat16).astype(jnp.float32)
    key_pos = jnp.arange(SEQ)
    hid_blocks = hidden.reshape(BATCH, n_blocks, Q_ROWS, D_MODEL).transpose(1, 0, 2, 3)
    grad_blocks = grad_out.reshape(BATCH, n_blocks, Q_ROWS, D_MODEL).transpose(1, 0, 2, 3)
    cos_blocks = cos_tab.reshape(n_blocks, Q_ROWS, HEAD_DIM // 2)
    sin_blocks = sin_tab.reshape(n_blocks, Q_ROWS, HEAD_DIM // 2)
    row_starts = jnp.arange(n_blocks) * Q_ROWS
    kv_zero = jnp.zeros((BATCH, SEQ, HEAD_DIM), jnp.float32)
    big_zero = jnp.zeros((BATCH, SEQ, D_MODEL), jnp.float32)

    def head_step(carry_in, head_weights):
        out_acc, dh_acc, dk_acc, dv_acc = carry_in
        wq_head, wo_head = head_weights

        def block_step(block_carry, block_in):
            dk_run, dv_run, dwq_run, dwo_run = block_carry
            hid_blk, grad_blk, cos_blk, sin_blk, row_start = block_in
            hid_flat = hid_blk.reshape(BATCH * Q_ROWS, D_MODEL)
            grad_flat = grad_blk.reshape(BATCH * Q_ROWS, D_MODEL)
            q_pre = jnp.dot(hid_flat, wq_head, preferred_element_type=jnp.float32).reshape(BATCH, Q_ROWS, HEAD_DIM)
            q_rot = (rotate(q_pre, cos_blk, sin_blk) * q_scale).astype(jnp.bfloat16).astype(jnp.float32)
            scores = jnp.einsum("bqe,bke->bqk", q_rot, key_rot)
            q_pos = row_start + jnp.arange(Q_ROWS)
            allowed = key_pos[None, :] <= q_pos[:, None]
            scores = jnp.where(allowed[None], scores, -jnp.inf)
            probs_blk = jax.nn.softmax(scores, axis=-1)
            attn_blk = jnp.einsum("bqk,bke->bqe", probs_blk, val_all).astype(jnp.bfloat16)
            d_attn = jnp.dot(grad_flat, wo_head.T, preferred_element_type=jnp.float32).astype(jnp.bfloat16)
            attn_f = attn_blk.astype(jnp.float32)
            d_attn_f = d_attn.astype(jnp.float32).reshape(BATCH, Q_ROWS, HEAD_DIM)
            d_prob = jnp.einsum("bqe,bke->bqk", d_attn_f, val_all)
            row_delta = jnp.sum(d_attn_f * attn_f, axis=-1, keepdims=True)
            d_score = probs_blk * (d_prob - row_delta)
            dq_blk = jnp.einsum("bqk,bke->bqe", d_score, key_rot)
            dk_run = dk_run + jnp.einsum("bqk,bqe->bke", d_score, q_rot)
            dv_run = dv_run + jnp.einsum("bqk,bqe->bke", probs_blk, d_attn_f)
            dq_pre = (unrotate(dq_blk, cos_blk, sin_blk) * q_scale).astype(jnp.bfloat16).reshape(BATCH * Q_ROWS, HEAD_DIM)
            attn_flat = attn_blk.reshape(BATCH * Q_ROWS, HEAD_DIM)
            dwq_run = dwq_run + jnp.dot(hid_flat.T, dq_pre, preferred_element_type=jnp.float32)
            dwo_run = dwo_run + jnp.dot(attn_flat.T, grad_flat, preferred_element_type=jnp.float32)
            out_part = jnp.dot(attn_flat, wo_head, preferred_element_type=jnp.float32)
            dh_part = jnp.dot(dq_pre, wq_head.T, preferred_element_type=jnp.float32)
            return (dk_run, dv_run, dwq_run, dwo_run), (out_part, dh_part)

        block_init = (kv_zero, kv_zero, jnp.zeros((D_MODEL, HEAD_DIM), jnp.float32), jnp.zeros((HEAD_DIM, D_MODEL), jnp.float32))
        block_out, block_ys = lax.scan(block_step, block_init, (hid_blocks, grad_blocks, cos_blocks, sin_blocks, row_starts))
        dk_run, dv_run, dwq_run, dwo_run = block_out
        out_parts, dh_parts = block_ys
        out_head = out_parts.reshape(n_blocks, BATCH, Q_ROWS, D_MODEL).transpose(1, 0, 2, 3).reshape(BATCH, SEQ, D_MODEL)
        dh_head = dh_parts.reshape(n_blocks, BATCH, Q_ROWS, D_MODEL).transpose(1, 0, 2, 3).reshape(BATCH, SEQ, D_MODEL)
        new_carry = (out_acc + out_head, dh_acc + dh_head, dk_acc + dk_run, dv_acc + dv_run)
        return new_carry, (dwq_run, dwo_run)

    head_init = (big_zero, big_zero, kv_zero, kv_zero)
    head_out, head_ys = lax.scan(head_step, head_init, (w_query.transpose(1, 0, 2), w_out))
    out_acc, dh_acc, dk_acc, dv_acc = head_out
    d_w_query = head_ys[0].transpose(1, 0, 2)
    d_w_out = head_ys[1]
    dk_pre = unrotate(dk_acc, cos_tab, sin_tab).astype(jnp.bfloat16).reshape(BATCH * SEQ, HEAD_DIM)
    dv_pre = dv_acc.astype(jnp.bfloat16).reshape(BATCH * SEQ, HEAD_DIM)
    d_w_key = jnp.dot(flat_hidden.T, dk_pre, preferred_element_type=jnp.float32)
    d_w_value = jnp.dot(flat_hidden.T, dv_pre, preferred_element_type=jnp.float32)
    dh_kv = jnp.dot(dk_pre, w_key.T, preferred_element_type=jnp.float32) + jnp.dot(dv_pre, w_value.T, preferred_element_type=jnp.float32)
    d_hidden = (dh_acc + dh_kv.reshape(BATCH, SEQ, D_MODEL)).astype(jnp.bfloat16)
    attn_out = out_acc.astype(jnp.bfloat16)
    return attn_out, d_hidden, d_w_query, d_w_key, d_w_value, d_w_out
```

```python
import functools

import jax
import jax.numpy as jnp
from jax import lax
from jax.experimental import pallas as pl
from jax.experimental.pallas import tpu as pltpu
from jax.sharding import PartitionSpec as P

ROPE_BASE = 10000.0
MESH = pl.DeviceIdType.MESH
TILE = 128
KBLK = 512
CHUNK = 256
VMEM_LIMIT = 60 * 1024 * 1024


def rope_tables(positions, head_dim):
    half_dim = head_dim // 2
    inv_freq = 1.0 / jnp.power(ROPE_BASE, jnp.arange(half_dim, dtype=jnp.float32) * (2.0 / head_dim))
    angles = positions.astype(jnp.float32)[:, None] * inv_freq[None, :]
    return jnp.cos(angles), jnp.sin(angles)


def rotate(rot_in, cos_tab, sin_tab):
    half_dim = rot_in.shape[-1] // 2
    low_half = rot_in[..., :half_dim]
    high_half = rot_in[..., half_dim:]
    return jnp.concatenate([low_half * cos_tab - high_half * sin_tab, high_half * cos_tab + low_half * sin_tab], axis=-1)


def unrotate(rot_in, cos_tab, sin_tab):
    return rotate(rot_in, cos_tab, -sin_tab)


def gather_kernel(n_arrays, shared, n_sums, *refs):
    n_in = n_arrays + n_sums
    ins, sum_ins = refs[:n_arrays], refs[n_arrays:n_in]
    outs, sum_outs = refs[n_in : n_in + n_arrays], refs[n_in + n_arrays : 2 * n_in]
    near, far = refs[2 * n_in : 2 * n_in + n_sums], refs[2 * n_in + n_sums : 2 * n_in + 2 * n_sums]
    send_sems, recv_sems, local_sems = refs[2 * n_in + 2 * n_sums : 2 * n_in + 2 * n_sums + 3]
    sum_sems = refs[2 * n_in + 2 * n_sums + 3 :]
    me, core = lax.axis_index("tp"), lax.axis_index("cp") % 2
    z_idx, y_idx = me // 2, me % 2
    right, left, part = me + 2, me - 2, z_idx * 2 + 1 - y_idx
    has_right, has_left = z_idx < 3, z_idx > 0
    sibling = lax.axis_index("cp") + 1 - 2 * core

    barrier = pltpu.get_barrier_semaphore()

    def greet(device):
        pl.semaphore_signal(barrier, inc=1, device_id=device, device_id_type=MESH)
        return None

    greet({"tp": part})
    across = (lax.axis_index("cp") + 2) % 4
    extra = 1
    if shared or n_sums:
        greet({"cp": sibling})
        extra += 1
    if n_sums:
        greet({"cp": across})
        extra += 1

    @pl.when(has_right)
    def _():
        greet({"tp": right})

    @pl.when(has_left)
    def _():
        greet({"tp": left})

    ends = jnp.where(has_right, 1, 0) + jnp.where(has_left, 1, 0)
    pl.semaphore_wait(barrier, ends + extra)

    def geometry(i):
        whole = outs[i].shape[0] // 8
        rows = whole // 2 if shared else whole
        return whole, rows, (core * rows if shared else 0)

    def segment(rows, seg):
        a_len = (rows // 12 + 8) // 16 * 16
        b_len = rows // 2 - a_len
        return {
            "A0": (0, a_len),
            "A1": (rows - a_len, a_len),
            "B": (a_len, 2 * b_len),
            "B0": (a_len, b_len),
            "B1": (rows // 2, b_len),
            "H0": (0, rows // 2),
            "H1": (rows // 2, rows // 2),
        }[seg]

    names = ["yA0", "yA1", "yB"] + [f"{kind}{s}{h}" for kind in ("R", "L", "yR", "yL", "pR", "pL") for s in range(3) for h in range(2)]
    index = {name: k for k, name in enumerate(names)}

    def describe(name, receiving):
        if name[:2] in ("yA", "yB") and len(name) <= 3:
            return name[1:], z_idx, (1 - y_idx if receiving else y_idx), part, None, not receiving
        kind, s, h = name[:-2], int(name[-2]), name[-1]
        sign = -1 if "R" in kind else 1
        if kind in ("yR", "yL"):
            z_src = z_idx + sign * (1 + s)
            ok = z_src >= 0 if sign < 0 else z_src < 4
            return "B" + h, z_src, (1 - y_idx if receiving else y_idx), part, ok, False
        seg = ("H" if len(kind) == 1 else "A") + h
        y_src = y_idx if len(kind) == 1 else 1 - y_idx
        if receiving:
            z_src = z_idx + sign * (1 + s)
            ok = z_src >= 0 if sign < 0 else z_src < 4
        else:
            z_src = z_idx + sign * s
            ok = (z_src >= 0) & has_right if sign < 0 else (z_src < 4) & has_left
        return seg, z_src, y_src, (right if sign < 0 else left), ok, len(kind) == 1 and s == 0 and not receiving

    def each(name, receiving, act):
        seg, z_src, y_src, target, ok, own = describe(name, receiving)

        def run():
            for i in range(n_arrays):
                whole, rows, offset = geometry(i)
                first, count = segment(rows, seg)
                span = pl.ds(pl.multiple_of((z_src * 2 + y_src) * whole + offset + first, 16), count)
                own_span = pl.ds(pl.multiple_of(offset + first, 16), count)
                act(
                    pltpu.make_async_remote_copy(
                        src_ref=ins[i].at[own_span] if own else outs[i].at[span],
                        dst_ref=outs[i].at[span],
                        send_sem=send_sems.at[i, index[name]],
                        recv_sem=recv_sems.at[i, index[name]],
                        device_id={"tp": target},
                        device_id_type=MESH,
                    )
                )

        if ok is None:
            run()
        else:
            pl.when(ok)(run)

    def start(*which):
        for name in which:
            each(name, False, lambda copy: copy.start())

    def arrive(*which):
        for name in which:
            each(name, True, lambda copy: copy.wait_recv())

    def half_of(i, which):
        half = sum_ins[i].shape[0] // 2
        return pl.ds(pl.multiple_of(which * half, 8), half)

    def sum_copy(i, stage):
        src = (sum_ins[i].at[half_of(i, 1 - core)], near[i], far[i])[stage]
        dst = (near[i], far[i], sum_outs[i].at[half_of(i, core)])[stage]
        return pltpu.make_async_remote_copy(
            src_ref=src,
            dst_ref=dst,
            send_sem=sum_sems[0].at[i, stage],
            recv_sem=sum_sems[1].at[i, stage],
            device_id={"cp": across if stage == 1 else sibling},
            device_id_type=MESH,
        )

    def sum_last(i):
        span = half_of(i, 1 - core)
        return pltpu.make_async_remote_copy(
            src_ref=far[i],
            dst_ref=sum_outs[i].at[span],
            send_sem=sum_sems[0].at[i, 2],
            recv_sem=sum_sems[1].at[i, 2],
            device_id={"cp": sibling},
            device_id_type=MESH,
        )

    def sum_store(i):
        return pltpu.make_async_copy(far[i], sum_outs[i].at[half_of(i, core)], sum_sems[2].at[i])

    def add_rows(dst, src, first):
        step = 32

        def body(n, carry):
            rows = pl.ds(pl.multiple_of(n * step, step), step)
            src_rows = pl.ds(pl.multiple_of(first + n * step, step), step)
            dst[rows, :] += src[src_rows, :]
            return carry

        lax.fori_loop(0, dst.shape[0] // step, body, 0)

    def sums_begin():
        for i in range(n_sums):
            sum_copy(i, 0).start()

    def sums_middle():
        for i in range(n_sums):
            sum_copy(i, 0).wait_recv()
            add_rows(near[i], sum_ins[i], core * (sum_ins[i].shape[0] // 2))
            sum_copy(i, 1).start()

    def sums_finish():
        for i in range(n_sums):
            sum_copy(i, 1).wait_recv()
            add_rows(far[i], near[i], 0)
            sum_copy(i, 2).start()
            sum_store(i).start()

    def sums_drain():
        for i in range(n_sums):
            sum_last(i).wait_recv()
            sum_store(i).wait()
            for stage in range(3):
                sum_copy(i, stage).wait_send()

    start("yA0", "R00", "L00", "yA1", "R01", "L01", "yB")
    sums_begin()
    own = []
    for i in range(n_arrays):
        whole, rows, offset = geometry(i)
        span = pl.ds(pl.multiple_of(me * whole + offset, 16), rows)
        own_span = pl.ds(pl.multiple_of(offset, 16), rows) if shared else pl.ds(0, rows)
        own.append(pltpu.make_async_copy(ins[i].at[own_span], outs[i].at[span], local_sems.at[i]))
        own[-1].start()
    for s in range(3):
        for h in "01":
            for side in "RL":
                arrive(f"{side}{s}{h}")
                if s < 2:
                    start(f"{side}{s + 1}{h}")
                start(f"y{side}{s}{h}")
        if s == 0:
            arrive("yA0", "yA1")
            sums_middle()
        for side in "RL":
            for h in "01":
                if s > 0:
                    arrive(f"p{side}{s - 1}{h}")
                start(f"p{side}{s}{h}")
    sums_finish()
    arrive("pR20", "pR21", "pL20", "pL21", "yB")
    for side in "RL":
        for s in range(3):
            for h in "01":
                arrive(f"y{side}{s}{h}")
    for name in names:
        each(name, False, lambda copy: copy.wait_send())
    for copy in own:
        copy.wait()
    sums_drain()
    if shared:
        last = len(names)
        swaps = []
        for i in range(n_arrays):
            whole, rows, offset = geometry(i)
            for block in range(8):
                span = pl.ds(pl.multiple_of(block * whole + offset, 16), rows)
                swaps.append(
                    pltpu.make_async_remote_copy(
                        src_ref=outs[i].at[span],
                        dst_ref=outs[i].at[span],
                        send_sem=send_sems.at[i, last + block],
                        recv_sem=recv_sems.at[i, last + block],
                        device_id={"cp": sibling},
                        device_id_type=MESH,
                    )
                )
                swaps[-1].start()
        for copy in swaps:
            copy.wait_send()
        for i in range(n_arrays):
            whole, rows, offset = geometry(i)
            for block in range(8):
                span = pl.ds(pl.multiple_of(block * whole + rows - offset, 16), rows)
                pltpu.make_async_remote_copy(
                    src_ref=outs[i].at[span],
                    dst_ref=outs[i].at[span],
                    send_sem=send_sems.at[i, last + block],
                    recv_sem=recv_sems.at[i, last + block],
                    device_id={"cp": sibling},
                    device_id_type=MESH,
                ).wait_recv()


def gather_tp(arrays, collective_id, shared=False, sums=()):
    n_arrays, n_sums = len(arrays), len(sums)
    n_steps = 3 + 6 * 6 + (8 if shared else 0)
    sent = sum(a.size * a.dtype.itemsize for a in arrays)
    dma = pltpu.SemaphoreType.DMA
    halves = [pltpu.VMEM((a.shape[0] // 2, a.shape[1]), a.dtype) for a in sums]
    return pl.pallas_call(
        functools.partial(gather_kernel, n_arrays, shared, n_sums),
        out_shape=[jax.ShapeDtypeStruct((8 * a.shape[0], a.shape[1]), a.dtype) for a in arrays]
        + [jax.ShapeDtypeStruct(a.shape, a.dtype) for a in sums],
        in_specs=[pl.BlockSpec(memory_space=pltpu.VMEM)] * (n_arrays + n_sums),
        out_specs=[pl.BlockSpec(memory_space=pl.ANY)] * (n_arrays + n_sums),
        scratch_shapes=halves
        + halves
        + [dma((n_arrays, n_steps)), dma((n_arrays, n_steps)), dma((n_arrays,))]
        + ([dma((n_sums, 3)), dma((n_sums, 3)), dma((n_sums,))] if n_sums else []),
        compiler_params=pltpu.CompilerParams(collective_id=collective_id, has_side_effects=True, vmem_limit_bytes=VMEM_LIMIT),
        cost_estimate=pl.CostEstimate(flops=sent * 20000, bytes_accessed=9 * sent, transcendentals=0),
        name=f"gather_tp_{collective_id}",
    )(*arrays, *sums)


N_CHUNK = 4


def reduce_kernel(part, out, acc, sib, side, back, tiles, ld_sem, s1_send, s1_recv, y_send, y_recv, x_send, x_recv, t_send, t_recv):
    me, cp_idx = lax.axis_index("tp"), lax.axis_index("cp")
    core, x_idx = cp_idx % 2, cp_idx // 2
    piece_len = acc.shape[2]
    chunk = piece_len // N_CHUNK
    partner = me + 1 - 2 * (me % 2)
    sibling = cp_idx + 1 - 2 * core
    across = cp_idx + 2 - 4 * x_idx
    straddles = (me == 2) | (me == 5)
    merges = (me == 3) | (me == 4)
    main_batch = (3 * me + 1) // 8

    def base(batch):
        return 5 * batch // 2

    def limit(batch):
        return (5 * batch + 7) // 2

    barrier = pltpu.get_barrier_semaphore()
    for step in range(1, 8):
        pl.semaphore_signal(barrier, inc=1, device_id={"tp": (me + step) % 8}, device_id_type=MESH)
    pl.semaphore_signal(barrier, inc=1, device_id={"cp": sibling}, device_id_type=MESH)
    pl.semaphore_signal(barrier, inc=1, device_id={"cp": across}, device_id_type=MESH)
    pl.semaphore_wait(barrier, 9)

    def piece(idx):
        return pl.ds(pl.multiple_of(idx * piece_len, piece_len), piece_len)

    def load(slot, k):
        return pltpu.make_async_copy(part.at[slot, piece(2 * k + core)], acc.at[slot, k], ld_sem.at[slot, k])

    def to_sibling(slot, k):
        return pltpu.make_async_remote_copy(
            src_ref=part.at[slot, piece(2 * k + 1 - core)],
            dst_ref=sib.at[slot, k],
            send_sem=s1_send.at[slot, k],
            recv_sem=s1_recv.at[slot, k],
            device_id={"cp": sibling},
            device_id_type=MESH,
        )

    def rows_of(c):
        return pl.ds(c * chunk, chunk)

    def to_partner(c):
        return pltpu.make_async_remote_copy(
            src_ref=acc.at[1, 0, rows_of(c)],
            dst_ref=side.at[rows_of(c)],
            send_sem=y_send.at[c],
            recv_sem=y_recv.at[c],
            device_id={"tp": partner},
            device_id_type=MESH,
        )

    def across_x(c):
        return pltpu.make_async_remote_copy(
            src_ref=acc.at[0, 0, rows_of(c)],
            dst_ref=back.at[rows_of(c)],
            send_sem=x_send.at[c],
            recv_sem=x_recv.at[c],
            device_id={"cp": across},
            device_id_type=MESH,
        )

    def to_owner(slot, i):
        batch = 1 if slot else main_batch
        tile = 8 * batch + i
        return pltpu.make_async_remote_copy(
            src_ref=acc.at[slot, x_idx, pl.ds(i * TILE, TILE)],
            dst_ref=tiles.at[me - base(batch), tile % 3],
            send_sem=t_send.at[slot, i],
            recv_sem=t_recv.at[me - base(batch), tile % 3],
            device_id={"tp": tile // 3},
            device_id_type=MESH,
        )

    def not_mine(slot, i):
        return (8 * (1 if slot else main_batch) + i) // 3 != me

    def for_slots(act):
        for k in range(2):
            for slot in range(2):
                conds = []
                if k == 1:
                    conds.append(x_idx == 1)
                if slot == 1:
                    conds.append(straddles)
                run = functools.partial(act, slot, k)
                if conds:
                    pl.when(functools.reduce(jnp.logical_and, conds))(run)
                else:
                    run()

    def begin(slot, k):
        to_sibling(slot, k).start()
        load(slot, k).start()

    def join(slot, k):
        load(slot, k).wait()
        to_sibling(slot, k).wait_recv()
        for c in range(N_CHUNK):
            acc[slot, k, rows_of(c)] += sib[slot, k, rows_of(c)]
        if slot == 1 and k == 0:
            @pl.when(x_idx == 1)
            def _():
                for c in range(N_CHUNK):
                    to_partner(c).start()

        if slot == 1:
            @pl.when(x_idx == k)
            def _():
                for i in range(piece_len // TILE):
                    pl.when(not_mine(1, i))(to_owner(1, i).start)

    for_slots(begin)
    for_slots(join)

    def finish(k, c):
        if k == 0:
            @pl.when(merges & (x_idx == 1))
            def _():
                to_partner(c).wait_recv()
                acc[0, 0, rows_of(c)] += side[rows_of(c)]

            @pl.when(x_idx == 1)
            def _():
                across_x(c).start()

            @pl.when(x_idx == 0)
            def _():
                across_x(c).wait_recv()
                acc[0, 0, rows_of(c)] += back[rows_of(c)]

        @pl.when(x_idx == k)
        def _():
            for i in range(c * chunk // TILE, (c + 1) * chunk // TILE):
                pl.when(not_mine(0, i))(to_owner(0, i).start)

    for c in range(N_CHUNK):
        finish(0, c)

    @pl.when(x_idx == 1)
    def _():
        for c in range(N_CHUNK):
            finish(1, c)

    for local in range(3):
        tile = 3 * me + local
        batch = tile // 8
        rows = pl.ds(local * TILE, TILE)
        first_rank = base(batch)
        out[rows, :] = jnp.zeros((TILE, out.shape[1]), jnp.float32)

        @pl.when(batch == main_batch)
        def _():
            out[rows, :] += acc[0, x_idx, pl.ds(pl.multiple_of((tile - 8 * batch) * TILE, TILE), TILE)]

        @pl.when(batch != main_batch)
        def _():
            out[rows, :] += acc[1, x_idx, pl.ds(pl.multiple_of((tile - 8 * batch) * TILE, TILE), TILE)]

        for rank in range(4):
            @pl.when((first_rank + rank < limit(batch)) & (first_rank + rank != me))
            def _():
                pltpu.make_async_remote_copy(
                    src_ref=tiles.at[rank, local],
                    dst_ref=tiles.at[rank, local],
                    send_sem=t_send.at[0, 0],
                    recv_sem=t_recv.at[rank, local],
                    device_id={"tp": partner},
                    device_id_type=MESH,
                ).wait_recv()
                out[rows, :] += tiles[rank, local]

    def drain(slot, k):
        to_sibling(slot, k).wait_send()
        if slot == 1 and k == 0:
            @pl.when(x_idx == 1)
            def _():
                for c in range(N_CHUNK):
                    to_partner(c).wait_send()

        if slot == 1:
            @pl.when(x_idx == k)
            def _():
                for i in range(piece_len // TILE):
                    pl.when(not_mine(1, i))(to_owner(1, i).wait_send)

    for_slots(drain)

    @pl.when(x_idx == 1)
    def _():
        for c in range(N_CHUNK):
            across_x(c).wait_send()

    for i in range(piece_len // TILE):
        pl.when(not_mine(0, i))(to_owner(0, i).wait_send)


def reduce_kv(part):
    n_slots, n_keys, width = part.shape
    piece_len = n_keys // 4
    dma = pltpu.SemaphoreType.DMA
    f32 = jnp.float32
    return pl.pallas_call(
        reduce_kernel,
        out_shape=jax.ShapeDtypeStruct((3 * TILE, width), f32),
        in_specs=[pl.BlockSpec(memory_space=pl.ANY)],
        out_specs=pl.BlockSpec(memory_space=pltpu.VMEM),
        scratch_shapes=[
            pltpu.VMEM((2, 2, piece_len, width), f32),
            pltpu.VMEM((2, 2, piece_len, width), f32),
            pltpu.VMEM((piece_len, width), f32),
            pltpu.VMEM((piece_len, width), f32),
            pltpu.VMEM((4, 3, TILE, width), f32),
            dma((2, 2)),
            dma((2, 2)),
            dma((2, 2)),
            dma((N_CHUNK,)),
            dma((N_CHUNK,)),
            dma((N_CHUNK,)),
            dma((N_CHUNK,)),
            dma((2, piece_len // TILE)),
            dma((4, 3)),
        ],
        compiler_params=pltpu.CompilerParams(collective_id=3, has_side_effects=True, vmem_limit_bytes=VMEM_LIMIT),
        cost_estimate=pl.CostEstimate(flops=20_000_000_000, bytes_accessed=30_000_000, transcendentals=0),
        name="reduce_kv",
    )(part)


def dot_nt(lhs, rhs):
    return lax.dot_general(lhs, rhs, (((1,), (1,)), ((), ())), preferred_element_type=jnp.float32)


def dot_nn(lhs, rhs):
    return lax.dot_general(lhs, rhs, (((1,), (0,)), ((), ())), preferred_element_type=jnp.float32)


def causal(shape, k_start, q_start):
    k_pos = k_start + lax.broadcasted_iota(jnp.int32, shape, 0)
    q_pos = q_start + lax.broadcasted_iota(jnp.int32, shape, 1) % TILE
    return k_pos <= q_pos


def forward_kernel(info, q_ref, k_ref, v_ref, o_ref, lse_ref, q_all, acc, run_max, run_sum):
    tile = pl.program_id(0)
    q_start = info[1, tile]
    last = q_start // KBLK
    head_dim = k_ref.shape[2]
    n_heads = q_ref.shape[1] // head_dim
    for head in range(n_heads):
        q_all[pl.ds(head * TILE, TILE), :] = q_ref[:, pl.ds(head * head_dim, head_dim)]
    acc[...] = jnp.zeros_like(acc)
    run_max[...] = jnp.full_like(run_max, -jnp.inf)
    run_sum[...] = jnp.zeros_like(run_sum)

    def block(k_idx, masked):
        k_start = pl.multiple_of(k_idx * KBLK, KBLK)
        key_blk = k_ref[0, pl.ds(k_start, KBLK), :]
        val_blk = v_ref[0, pl.ds(k_start, KBLK), :].T
        for chunk in range(n_heads * TILE // CHUNK):
            rows = pl.ds(chunk * CHUNK, CHUNK)
            scores = dot_nt(key_blk, q_all[rows, :])
            if masked:
                scores = jnp.where(causal(scores.shape, k_start, q_start), scores, -jnp.inf)
            old_max = run_max[:, rows]
            new_max = jnp.maximum(old_max, jnp.max(scores, axis=0, keepdims=True))
            rescale = jnp.exp(old_max - new_max)
            weights = jnp.exp(scores - new_max)
            run_max[:, rows] = new_max
            run_sum[:, rows] = run_sum[:, rows] * rescale + jnp.sum(weights, axis=0, keepdims=True)
            acc[:, rows] = acc[:, rows] * rescale + dot_nn(val_blk, weights.astype(jnp.bfloat16))

    def body(k_idx, carry):
        block(k_idx, False)
        return carry

    lax.fori_loop(0, last, body, 0)
    block(last, True)
    lse_ref[0] = run_max[...] + jnp.log(run_sum[...])
    inv_sum = 1.0 / run_sum[...]
    for head in range(n_heads):
        rows = pl.ds(head * TILE, TILE)
        o_ref[:, pl.ds(head * head_dim, head_dim)] = (acc[:, rows] * inv_sum[:, head * TILE : (head + 1) * TILE]).T.astype(jnp.bfloat16)


def backward_kernel(info, q_ref, do_ref, lse_ref, delta_ref, k_ref, v_ref, dq_ref, dkv_ref, q_all, do_all, dq_acc):
    tile = pl.program_id(0)
    q_start = info[1, tile]
    last = q_start // KBLK
    head_dim = k_ref.shape[2]
    n_heads = q_ref.shape[1] // head_dim
    for head in range(n_heads):
        q_all[pl.ds(head * TILE, TILE), :] = q_ref[:, pl.ds(head * head_dim, head_dim)]
        do_all[pl.ds(head * TILE, TILE), :] = do_ref[:, pl.ds(head * head_dim, head_dim)]
    dq_acc[...] = jnp.zeros_like(dq_acc)

    @pl.when(info[3, tile] == 1)
    def _():
        dkv_ref[...] = jnp.zeros_like(dkv_ref)

    def block(k_idx, masked):
        k_start = pl.multiple_of(k_idx * KBLK, KBLK)
        keys = pl.ds(k_start, KBLK)
        key_blk = k_ref[0, keys, :]
        val_blk = v_ref[0, keys, :]
        keyt_blk = key_blk.T
        dk_part = jnp.zeros((KBLK, head_dim), jnp.float32)
        dv_part = jnp.zeros((KBLK, head_dim), jnp.float32)
        for chunk in range(n_heads * TILE // CHUNK):
            rows = pl.ds(chunk * CHUNK, CHUNK)
            q_rows, do_rows = q_all[rows, :], do_all[rows, :]
            probs = jnp.exp(dot_nt(key_blk, q_rows) - lse_ref[0, :, rows])
            if masked:
                probs = jnp.where(causal(probs.shape, k_start, q_start), probs, 0.0)
            d_score = (probs * (dot_nt(val_blk, do_rows) - delta_ref[0, :, rows])).astype(jnp.bfloat16)
            dv_part += dot_nn(probs.astype(jnp.bfloat16), do_rows)
            dk_part += dot_nn(d_score, q_rows)
            dq_acc[:, rows] += dot_nn(keyt_blk, d_score)
        dkv_ref[0, keys, pl.ds(0, head_dim)] += dk_part
        dkv_ref[0, keys, pl.ds(head_dim, head_dim)] += dv_part

    def body(k_idx, carry):
        block(k_idx, False)
        return carry

    lax.fori_loop(0, last, body, 0)
    block(last, True)
    for head in range(n_heads):
        dq_ref[:, pl.ds(head * head_dim, head_dim)] = dq_acc[:, pl.ds(head * TILE, TILE)].T


def attention_forward(info, queries, kv_all):
    n_rows, width = queries.shape
    n_keys, head_dim = kv_all.shape[1], kv_all.shape[2] // 2
    all_rows = width // head_dim * TILE
    return pl.pallas_call(
        forward_kernel,
        out_shape=[
            jax.ShapeDtypeStruct((n_rows, width), jnp.bfloat16),
            jax.ShapeDtypeStruct((n_rows // TILE, 1, all_rows), jnp.float32),
        ],
        grid_spec=pltpu.PrefetchScalarGridSpec(
            num_scalar_prefetch=1,
            grid=(n_rows // TILE,),
            in_specs=[
                pl.BlockSpec((TILE, width), lambda i, info: (i, 0)),
                pl.BlockSpec((1, n_keys, head_dim), lambda i, info: (info[0, i], 0, 0)),
                pl.BlockSpec((1, n_keys, head_dim), lambda i, info: (info[0, i], 0, 1)),
            ],
            out_specs=[
                pl.BlockSpec((TILE, width), lambda i, info: (i, 0)),
                pl.BlockSpec((1, 1, all_rows), lambda i, info: (i, 0, 0)),
            ],
            scratch_shapes=[
                pltpu.VMEM((all_rows, head_dim), jnp.bfloat16),
                pltpu.VMEM((head_dim, all_rows), jnp.float32),
                pltpu.VMEM((1, all_rows), jnp.float32),
                pltpu.VMEM((1, all_rows), jnp.float32),
            ],
        ),
        compiler_params=pltpu.CompilerParams(vmem_limit_bytes=VMEM_LIMIT),
        cost_estimate=pl.CostEstimate(flops=8_000_000_000, bytes_accessed=10_000_000, transcendentals=6_000_000),
        name="attention_forward",
    )(info, queries, kv_all, kv_all)


def attention_backward(info, queries, d_out, row_lse, row_delta, kv_all):
    n_rows, width = queries.shape
    n_keys, head_dim = kv_all.shape[1], kv_all.shape[2] // 2
    all_rows = width // head_dim * TILE
    return pl.pallas_call(
        backward_kernel,
        out_shape=[
            jax.ShapeDtypeStruct((n_rows, width), jnp.float32),
            jax.ShapeDtypeStruct((2, n_keys, 2 * head_dim), jnp.float32),
        ],
        grid_spec=pltpu.PrefetchScalarGridSpec(
            num_scalar_prefetch=1,
            grid=(n_rows // TILE,),
            in_specs=[
                pl.BlockSpec((TILE, width), lambda i, info: (i, 0)),
                pl.BlockSpec((TILE, width), lambda i, info: (i, 0)),
                pl.BlockSpec((1, 1, all_rows), lambda i, info: (i, 0, 0)),
                pl.BlockSpec((1, 1, all_rows), lambda i, info: (i, 0, 0)),
                pl.BlockSpec((1, n_keys, head_dim), lambda i, info: (info[0, i], 0, 0)),
                pl.BlockSpec((1, n_keys, head_dim), lambda i, info: (info[0, i], 0, 1)),
            ],
            out_specs=[
                pl.BlockSpec((TILE, width), lambda i, info: (i, 0)),
                pl.BlockSpec((1, n_keys, 2 * head_dim), lambda i, info: (info[2, i], 0, 0)),
            ],
            scratch_shapes=[
                pltpu.VMEM((all_rows, head_dim), jnp.bfloat16),
                pltpu.VMEM((all_rows, head_dim), jnp.bfloat16),
                pltpu.VMEM((head_dim, all_rows), jnp.float32),
            ],
        ),
        compiler_params=pltpu.CompilerParams(vmem_limit_bytes=VMEM_LIMIT),
        cost_estimate=pl.CostEstimate(flops=20_000_000_000, bytes_accessed=20_000_000, transcendentals=6_000_000),
        name="attention_backward",
    )(info, queries, d_out, row_lse, row_delta, kv_all, kv_all)


def solution(mesh):
    tp_size, cp_size = mesh.shape["tp"], mesh.shape["cp"]

    def local_program(hidden, grad_out, w_query, w_key, w_value, w_out):
        n_batch, block_len, width = hidden.shape
        head_dim = w_key.shape[1]
        n_heads = tp_size
        q_scale = head_dim ** -0.5
        tp_idx, cp_idx = lax.axis_index("tp"), lax.axis_index("cp")
        n_tokens = n_batch * block_len
        n_rows = n_tokens // tp_size
        row0 = tp_idx * n_rows
        hid_flat = hidden.reshape(n_tokens, width)
        grad_flat = grad_out.reshape(n_tokens, width)
        hid_own = lax.dynamic_slice_in_dim(hid_flat, row0, n_rows, 0)
        grad_own = lax.dynamic_slice_in_dim(grad_flat, row0, n_rows, 0)

        cos_piece, sin_piece = rope_tables(cp_idx * block_len + jnp.arange(block_len), head_dim)
        key_pre = jnp.einsum("bsd,de->bse", hidden, w_key, preferred_element_type=jnp.float32)
        key_loc = rotate(key_pre, cos_piece, sin_piece).astype(jnp.bfloat16)
        val_loc = jnp.einsum("bsd,de->bse", hidden, w_value, preferred_element_type=jnp.float32).astype(jnp.bfloat16)
        kv_loc = jnp.concatenate([key_loc, val_loc], axis=-1)
        kv_all = lax.all_gather(kv_loc, "cp", axis=1, tiled=True)

        wq_all, wo_all = gather_tp([w_query.reshape(width, head_dim), w_out.reshape(head_dim, width)], 0, shared=True)
        wq_all = wq_all.reshape(n_heads, width, head_dim)

        own_pos = cp_idx * block_len + (row0 + jnp.arange(n_rows)) % block_len
        cos_own, sin_own = rope_tables(own_pos, head_dim)
        cos_q, sin_q = cos_own[:, None, :], sin_own[:, None, :]
        q_pre = jnp.einsum("rd,nde->rne", hid_own, wq_all, preferred_element_type=jnp.float32)
        queries = (rotate(q_pre, cos_q, sin_q) * q_scale).astype(jnp.bfloat16).reshape(n_rows, n_heads * head_dim)
        d_out = jnp.einsum("rd,fd->rf", grad_own, wo_all, preferred_element_type=jnp.float32).astype(jnp.bfloat16)

        n_tiles = n_rows // TILE
        tile_ids = tp_idx * n_tiles + jnp.arange(n_tiles)
        per_batch = block_len // TILE
        tile_batch = tile_ids // per_batch
        tile_slot = (tile_batch != tile_batch[1]).astype(tile_ids.dtype)
        fresh = jnp.concatenate([jnp.ones((1,), tile_slot.dtype), jnp.abs(tile_slot[1:] - tile_slot[:-1])])
        info = jnp.stack([tile_batch, cp_idx * block_len + tile_ids % per_batch * TILE, tile_slot, fresh]).astype(jnp.int32)

        attn_own, row_lse = attention_forward(info, queries, kv_all)
        row_delta = jnp.einsum("rne,rne->rn", d_out.reshape(n_rows, n_heads, head_dim), attn_own.reshape(n_rows, n_heads, head_dim), preferred_element_type=jnp.float32)
        row_delta = row_delta.reshape(n_tiles, TILE, n_heads).transpose(0, 2, 1).reshape(n_tiles, 1, n_heads * TILE)
        dq_own, dkv_slots = attention_backward(info, queries, d_out, row_lse, row_delta, kv_all)
        dq_pre = (unrotate(dq_own.reshape(n_rows, n_heads, head_dim), cos_q, sin_q) * q_scale).astype(jnp.bfloat16)

        dkv_own = reduce_kv(dkv_slots)
        dk_own = unrotate(dkv_own[:, :head_dim], cos_own, sin_own).astype(jnp.bfloat16)
        dv_own = dkv_own[:, head_dim:].astype(jnp.bfloat16)

        dkv_piece, attn_all = gather_tp([jnp.concatenate([dk_own, dv_own], axis=-1), attn_own], 1)
        attn_head = lax.dynamic_slice_in_dim(attn_all, tp_idx * head_dim, head_dim, 1)
        d_w_out = jnp.einsum("rf,rd->fd", attn_head, grad_flat, preferred_element_type=jnp.float32)
        d_w_kv = jnp.einsum("rd,rf->df", hid_flat, dkv_piece, preferred_element_type=jnp.float32)
        dq_all, d_w_out, d_w_kv = gather_tp([dq_pre.reshape(n_rows, n_heads * head_dim)], 2, sums=[d_w_out, d_w_kv])
        dq_head = lax.dynamic_slice_in_dim(dq_all, tp_idx * head_dim, head_dim, 1)
        d_w_query = lax.psum(jnp.einsum("rd,rf->df", hid_flat, dq_head, preferred_element_type=jnp.float32), "cp")
        attn_out = jnp.einsum("rf,fd->rd", attn_all, wo_all, preferred_element_type=jnp.float32).astype(jnp.bfloat16)
        d_hidden = jnp.einsum("rne,nde->rd", dq_all.reshape(n_tokens, n_heads, head_dim), wq_all, preferred_element_type=jnp.float32)
        d_hidden += jnp.einsum("rf,df->rd", dkv_piece, jnp.concatenate([w_key, w_value], axis=1), preferred_element_type=jnp.float32)
        return (
            attn_out.reshape(hidden.shape),
            d_hidden.astype(jnp.bfloat16).reshape(hidden.shape),
            d_w_query[:, None, :],
            d_w_kv[:, :head_dim],
            d_w_kv[:, head_dim:],
            d_w_out[None],
        )

    row_spec = P(None, "cp", None)
    return jax.shard_map(local_program, mesh=mesh, in_specs=(row_spec, row_spec, P(None, "tp", None), P(), P(), P("tp", None, None)), out_specs=(row_spec, row_spec, P(None, "tp", None), P(), P(), P("tp", None, None)), check_vma=False)
```

```python
import functools

import jax
import jax.numpy as jnp
from jax import lax
from jax.experimental import pallas as pl
from jax.experimental.pallas import tpu as pltpu
from jax.sharding import PartitionSpec as P

ROPE_BASE = 10000.0
MESH = pl.DeviceIdType.MESH
TILE = 128
KBLK = 512
CHUNK = 256
VMEM_LIMIT = 60 * 1024 * 1024


def rope_tables(positions, head_dim):
    half_dim = head_dim // 2
    inv_freq = 1.0 / jnp.power(ROPE_BASE, jnp.arange(half_dim, dtype=jnp.float32) * (2.0 / head_dim))
    angles = positions.astype(jnp.float32)[:, None] * inv_freq[None, :]
    return jnp.cos(angles), jnp.sin(angles)


def rotate(rot_in, cos_tab, sin_tab):
    half_dim = rot_in.shape[-1] // 2
    low_half = rot_in[..., :half_dim]
    high_half = rot_in[..., half_dim:]
    return jnp.concatenate([low_half * cos_tab - high_half * sin_tab, high_half * cos_tab + low_half * sin_tab], axis=-1)


def unrotate(rot_in, cos_tab, sin_tab):
    return rotate(rot_in, cos_tab, -sin_tab)


def gather_kernel(n_arrays, shared, n_sums, *refs):
    n_in = n_arrays + n_sums
    ins, sum_ins = refs[:n_arrays], refs[n_arrays:n_in]
    outs, sum_outs = refs[n_in : n_in + n_arrays], refs[n_in + n_arrays : 2 * n_in]
    near, far = refs[2 * n_in : 2 * n_in + n_sums], refs[2 * n_in + n_sums : 2 * n_in + 2 * n_sums]
    send_sems, recv_sems, local_sems = refs[2 * n_in + 2 * n_sums : 2 * n_in + 2 * n_sums + 3]
    sum_sems = refs[2 * n_in + 2 * n_sums + 3 :]
    me, core = lax.axis_index("tp"), lax.axis_index("cp") % 2
    z_idx, y_idx = me // 2, me % 2
    right, left, part = me + 2, me - 2, z_idx * 2 + 1 - y_idx
    has_right, has_left = z_idx < 3, z_idx > 0
    sibling = lax.axis_index("cp") + 1 - 2 * core

    barrier = pltpu.get_barrier_semaphore()

    def greet(device):
        pl.semaphore_signal(barrier, inc=1, device_id=device, device_id_type=MESH)
        return None

    greet({"tp": part})
    across = (lax.axis_index("cp") + 2) % 4
    extra = 1
    if shared or n_sums:
        greet({"cp": sibling})
        extra += 1
    if n_sums:
        greet({"cp": across})
        extra += 1

    @pl.when(has_right)
    def _():
        greet({"tp": right})

    @pl.when(has_left)
    def _():
        greet({"tp": left})

    ends = jnp.where(has_right, 1, 0) + jnp.where(has_left, 1, 0)
    pl.semaphore_wait(barrier, ends + extra)

    def geometry(i):
        whole = outs[i].shape[0] // 8
        rows = whole // 2 if shared else whole
        return whole, rows, (core * rows if shared else 0)

    def segment(rows, seg):
        a_len = (rows // 12 + 8) // 16 * 16
        b_len = rows // 2 - a_len
        return {
            "A0": (0, a_len),
            "A1": (rows - a_len, a_len),
            "B": (a_len, 2 * b_len),
            "B0": (a_len, b_len),
            "B1": (rows // 2, b_len),
            "H0": (0, rows // 2),
            "H1": (rows // 2, rows // 2),
        }[seg]

    names = ["yA0", "yA1", "yB"] + [f"{kind}{s}{h}" for kind in ("R", "L", "yR", "yL", "pR", "pL") for s in range(3) for h in range(2)]
    index = {name: k for k, name in enumerate(names)}

    def describe(name, receiving):
        if name[:2] in ("yA", "yB") and len(name) <= 3:
            return name[1:], z_idx, (1 - y_idx if receiving else y_idx), part, None, not receiving
        kind, s, h = name[:-2], int(name[-2]), name[-1]
        sign = -1 if "R" in kind else 1
        if kind in ("yR", "yL"):
            z_src = z_idx + sign * (1 + s)
            ok = z_src >= 0 if sign < 0 else z_src < 4
            return "B" + h, z_src, (1 - y_idx if receiving else y_idx), part, ok, False
        seg = ("H" if len(kind) == 1 else "A") + h
        y_src = y_idx if len(kind) == 1 else 1 - y_idx
        if receiving:
            z_src = z_idx + sign * (1 + s)
            ok = z_src >= 0 if sign < 0 else z_src < 4
        else:
            z_src = z_idx + sign * s
            ok = (z_src >= 0) & has_right if sign < 0 else (z_src < 4) & has_left
        return seg, z_src, y_src, (right if sign < 0 else left), ok, len(kind) == 1 and s == 0 and not receiving

    def each(name, receiving, act):
        seg, z_src, y_src, target, ok, own = describe(name, receiving)

        def run():
            for i in range(n_arrays):
                whole, rows, offset = geometry(i)
                first, count = segment(rows, seg)
                span = pl.ds(pl.multiple_of((z_src * 2 + y_src) * whole + offset + first, 16), count)
                own_span = pl.ds(pl.multiple_of(offset + first, 16), count)
                act(
                    pltpu.make_async_remote_copy(
                        src_ref=ins[i].at[own_span] if own else outs[i].at[span],
                        dst_ref=outs[i].at[span],
                        send_sem=send_sems.at[i, index[name]],
                        recv_sem=recv_sems.at[i, index[name]],
                        device_id={"tp": target},
                        device_id_type=MESH,
                    )
                )

        if ok is None:
            run()
        else:
            pl.when(ok)(run)

    def start(*which):
        for name in which:
            each(name, False, lambda copy: copy.start())

    def arrive(*which):
        for name in which:
            each(name, True, lambda copy: copy.wait_recv())

    def half_of(i, which):
        half = sum_ins[i].shape[0] // 2
        return pl.ds(pl.multiple_of(which * half, 8), half)

    def sum_copy(i, stage):
        src = (sum_ins[i].at[half_of(i, 1 - core)], near[i], far[i])[stage]
        dst = (near[i], far[i], sum_outs[i].at[half_of(i, core)])[stage]
        return pltpu.make_async_remote_copy(
            src_ref=src,
            dst_ref=dst,
            send_sem=sum_sems[0].at[i, stage],
            recv_sem=sum_sems[1].at[i, stage],
            device_id={"cp": across if stage == 1 else sibling},
            device_id_type=MESH,
        )

    def sum_last(i):
        span = half_of(i, 1 - core)
        return pltpu.make_async_remote_copy(
            src_ref=far[i],
            dst_ref=sum_outs[i].at[span],
            send_sem=sum_sems[0].at[i, 2],
            recv_sem=sum_sems[1].at[i, 2],
            device_id={"cp": sibling},
            device_id_type=MESH,
        )

    def sum_store(i):
        return pltpu.make_async_copy(far[i], sum_outs[i].at[half_of(i, core)], sum_sems[2].at[i])

    def add_rows(dst, src, first):
        step = 32

        def body(n, carry):
            rows = pl.ds(pl.multiple_of(n * step, step), step)
            src_rows = pl.ds(pl.multiple_of(first + n * step, step), step)
            dst[rows, :] += src[src_rows, :]
            return carry

        lax.fori_loop(0, dst.shape[0] // step, body, 0)

    def sums_begin():
        for i in range(n_sums):
            sum_copy(i, 0).start()

    def sums_middle():
        for i in range(n_sums):
            sum_copy(i, 0).wait_recv()
            add_rows(near[i], sum_ins[i], core * (sum_ins[i].shape[0] // 2))
            sum_copy(i, 1).start()

    def sums_finish():
        for i in range(n_sums):
            sum_copy(i, 1).wait_recv()
            add_rows(far[i], near[i], 0)
            sum_copy(i, 2).start()
            sum_store(i).start()

    def sums_drain():
        for i in range(n_sums):
            sum_last(i).wait_recv()
            sum_store(i).wait()
            for stage in range(3):
                sum_copy(i, stage).wait_send()

    start("yA0", "R00", "L00", "yA1", "R01", "L01", "yB")
    sums_begin()
    own = []
    for i in range(n_arrays):
        whole, rows, offset = geometry(i)
        span = pl.ds(pl.multiple_of(me * whole + offset, 16), rows)
        own_span = pl.ds(pl.multiple_of(offset, 16), rows) if shared else pl.ds(0, rows)
        own.append(pltpu.make_async_copy(ins[i].at[own_span], outs[i].at[span], local_sems.at[i]))
        own[-1].start()
    for s in range(3):
        for h in "01":
            for side in "RL":
                arrive(f"{side}{s}{h}")
                if s < 2:
                    start(f"{side}{s + 1}{h}")
                start(f"y{side}{s}{h}")
        if s == 0:
            arrive("yA0", "yA1")
            sums_middle()
        for side in "RL":
            for h in "01":
                if s > 0:
                    arrive(f"p{side}{s - 1}{h}")
                start(f"p{side}{s}{h}")
    sums_finish()
    arrive("pR20", "pR21", "pL20", "pL21", "yB")
    for side in "RL":
        for s in range(3):
            for h in "01":
                arrive(f"y{side}{s}{h}")
    for name in names:
        each(name, False, lambda copy: copy.wait_send())
    for copy in own:
        copy.wait()
    sums_drain()
    if shared:
        last = len(names)
        swaps = []
        for i in range(n_arrays):
            whole, rows, offset = geometry(i)
            for block in range(8):
                span = pl.ds(pl.multiple_of(block * whole + offset, 16), rows)
                swaps.append(
                    pltpu.make_async_remote_copy(
                        src_ref=outs[i].at[span],
                        dst_ref=outs[i].at[span],
                        send_sem=send_sems.at[i, last + block],
                        recv_sem=recv_sems.at[i, last + block],
                        device_id={"cp": sibling},
                        device_id_type=MESH,
                    )
                )
                swaps[-1].start()
        for copy in swaps:
            copy.wait_send()
        for i in range(n_arrays):
            whole, rows, offset = geometry(i)
            for block in range(8):
                span = pl.ds(pl.multiple_of(block * whole + rows - offset, 16), rows)
                pltpu.make_async_remote_copy(
                    src_ref=outs[i].at[span],
                    dst_ref=outs[i].at[span],
                    send_sem=send_sems.at[i, last + block],
                    recv_sem=recv_sems.at[i, last + block],
                    device_id={"cp": sibling},
                    device_id_type=MESH,
                ).wait_recv()


def gather_tp(arrays, collective_id, shared=False, sums=()):
    n_arrays, n_sums = len(arrays), len(sums)
    n_steps = 3 + 6 * 6 + (8 if shared else 0)
    sent = sum(a.size * a.dtype.itemsize for a in arrays)
    dma = pltpu.SemaphoreType.DMA
    halves = [pltpu.VMEM((a.shape[0] // 2, a.shape[1]), a.dtype) for a in sums]
    return pl.pallas_call(
        functools.partial(gather_kernel, n_arrays, shared, n_sums),
        out_shape=[jax.ShapeDtypeStruct((8 * a.shape[0], a.shape[1]), a.dtype) for a in arrays]
        + [jax.ShapeDtypeStruct(a.shape, a.dtype) for a in sums],
        in_specs=[pl.BlockSpec(memory_space=pltpu.VMEM)] * (n_arrays + n_sums),
        out_specs=[pl.BlockSpec(memory_space=pl.ANY)] * (n_arrays + n_sums),
        scratch_shapes=halves
        + halves
        + [dma((n_arrays, n_steps)), dma((n_arrays, n_steps)), dma((n_arrays,))]
        + ([dma((n_sums, 3)), dma((n_sums, 3)), dma((n_sums,))] if n_sums else []),
        compiler_params=pltpu.CompilerParams(collective_id=collective_id, has_side_effects=True, vmem_limit_bytes=VMEM_LIMIT),
        cost_estimate=pl.CostEstimate(flops=sent * 20000, bytes_accessed=9 * sent, transcendentals=0),
        name=f"gather_tp_{collective_id}",
    )(*arrays, *sums)


N_CHUNK = 4


def reduce_kernel(part, out, acc, sib, side, back, tiles, ld_sem, s1_send, s1_recv, y_send, y_recv, x_send, x_recv, t_send, t_recv):
    me, cp_idx = lax.axis_index("tp"), lax.axis_index("cp")
    core, x_idx = cp_idx % 2, cp_idx // 2
    piece_len = acc.shape[2]
    chunk = piece_len // N_CHUNK
    partner = me + 1 - 2 * (me % 2)
    sibling = cp_idx + 1 - 2 * core
    across = cp_idx + 2 - 4 * x_idx
    straddles = (me == 2) | (me == 5)
    merges = (me == 3) | (me == 4)
    main_batch = (3 * me + 1) // 8

    def base(batch):
        return 5 * batch // 2

    def limit(batch):
        return (5 * batch + 7) // 2

    barrier = pltpu.get_barrier_semaphore()
    for step in range(1, 8):
        pl.semaphore_signal(barrier, inc=1, device_id={"tp": (me + step) % 8}, device_id_type=MESH)
    pl.semaphore_signal(barrier, inc=1, device_id={"cp": sibling}, device_id_type=MESH)
    pl.semaphore_signal(barrier, inc=1, device_id={"cp": across}, device_id_type=MESH)
    pl.semaphore_wait(barrier, 9)

    def piece(idx):
        return pl.ds(pl.multiple_of(idx * piece_len, piece_len), piece_len)

    def load(slot, k):
        return pltpu.make_async_copy(part.at[slot, piece(2 * k + core)], acc.at[slot, k], ld_sem.at[slot, k])

    def to_sibling(slot, k):
        return pltpu.make_async_remote_copy(
            src_ref=part.at[slot, piece(2 * k + 1 - core)],
            dst_ref=sib.at[slot, k],
            send_sem=s1_send.at[slot, k],
            recv_sem=s1_recv.at[slot, k],
            device_id={"cp": sibling},
            device_id_type=MESH,
        )

    def rows_of(c):
        return pl.ds(c * chunk, chunk)

    def to_partner(c):
        return pltpu.make_async_remote_copy(
            src_ref=acc.at[1, 0, rows_of(c)],
            dst_ref=side.at[rows_of(c)],
            send_sem=y_send.at[c],
            recv_sem=y_recv.at[c],
            device_id={"tp": partner},
            device_id_type=MESH,
        )

    def across_x(c):
        return pltpu.make_async_remote_copy(
            src_ref=acc.at[0, 0, rows_of(c)],
            dst_ref=back.at[rows_of(c)],
            send_sem=x_send.at[c],
            recv_sem=x_recv.at[c],
            device_id={"cp": across},
            device_id_type=MESH,
        )

    def to_owner(slot, i):
        batch = 1 if slot else main_batch
        tile = 8 * batch + i
        return pltpu.make_async_remote_copy(
            src_ref=acc.at[slot, x_idx, pl.ds(i * TILE, TILE)],
            dst_ref=tiles.at[me - base(batch), tile % 3],
            send_sem=t_send.at[slot, i],
            recv_sem=t_recv.at[me - base(batch), tile % 3],
            device_id={"tp": tile // 3},
            device_id_type=MESH,
        )

    def not_mine(slot, i):
        return (8 * (1 if slot else main_batch) + i) // 3 != me

    def for_slots(act):
        for k in range(2):
            for slot in range(2):
                conds = []
                if k == 1:
                    conds.append(x_idx == 1)
                if slot == 1:
                    conds.append(straddles)
                run = functools.partial(act, slot, k)
                if conds:
                    pl.when(functools.reduce(jnp.logical_and, conds))(run)
                else:
                    run()

    def begin(slot, k):
        to_sibling(slot, k).start()
        load(slot, k).start()

    def join(slot, k):
        load(slot, k).wait()
        to_sibling(slot, k).wait_recv()
        for c in range(N_CHUNK):
            acc[slot, k, rows_of(c)] += sib[slot, k, rows_of(c)]
        if slot == 1 and k == 0:
            @pl.when(x_idx == 1)
            def _():
                for c in range(N_CHUNK):
                    to_partner(c).start()

        if slot == 1:
            @pl.when(x_idx == k)
            def _():
                for i in range(piece_len // TILE):
                    pl.when(not_mine(1, i))(to_owner(1, i).start)

    for_slots(begin)
    for_slots(join)

    def finish(k, c):
        if k == 0:
            @pl.when(merges & (x_idx == 1))
            def _():
                to_partner(c).wait_recv()
                acc[0, 0, rows_of(c)] += side[rows_of(c)]

            @pl.when(x_idx == 1)
            def _():
                across_x(c).start()

            @pl.when(x_idx == 0)
            def _():
                across_x(c).wait_recv()
                acc[0, 0, rows_of(c)] += back[rows_of(c)]

        @pl.when(x_idx == k)
        def _():
            for i in range(c * chunk // TILE, (c + 1) * chunk // TILE):
                pl.when(not_mine(0, i))(to_owner(0, i).start)

    for c in range(N_CHUNK):
        finish(0, c)

    @pl.when(x_idx == 1)
    def _():
        for c in range(N_CHUNK):
            finish(1, c)

    for local in range(3):
        tile = 3 * me + local
        batch = tile // 8
        rows = pl.ds(local * TILE, TILE)
        first_rank = base(batch)
        out[rows, :] = jnp.zeros((TILE, out.shape[1]), jnp.float32)

        @pl.when(batch == main_batch)
        def _():
            out[rows, :] += acc[0, x_idx, pl.ds(pl.multiple_of((tile - 8 * batch) * TILE, TILE), TILE)]

        @pl.when(batch != main_batch)
        def _():
            out[rows, :] += acc[1, x_idx, pl.ds(pl.multiple_of((tile - 8 * batch) * TILE, TILE), TILE)]

        for rank in range(4):
            @pl.when((first_rank + rank < limit(batch)) & (first_rank + rank != me))
            def _():
                pltpu.make_async_remote_copy(
                    src_ref=tiles.at[rank, local],
                    dst_ref=tiles.at[rank, local],
                    send_sem=t_send.at[0, 0],
                    recv_sem=t_recv.at[rank, local],
                    device_id={"tp": partner},
                    device_id_type=MESH,
                ).wait_recv()
                out[rows, :] += tiles[rank, local]

    def drain(slot, k):
        to_sibling(slot, k).wait_send()
        if slot == 1 and k == 0:
            @pl.when(x_idx == 1)
            def _():
                for c in range(N_CHUNK):
                    to_partner(c).wait_send()

        if slot == 1:
            @pl.when(x_idx == k)
            def _():
                for i in range(piece_len // TILE):
                    pl.when(not_mine(1, i))(to_owner(1, i).wait_send)

    for_slots(drain)

    @pl.when(x_idx == 1)
    def _():
        for c in range(N_CHUNK):
            across_x(c).wait_send()

    for i in range(piece_len // TILE):
        pl.when(not_mine(0, i))(to_owner(0, i).wait_send)


def reduce_kv(part):
    n_slots, n_keys, width = part.shape
    piece_len = n_keys // 4
    dma = pltpu.SemaphoreType.DMA
    f32 = jnp.float32
    return pl.pallas_call(
        reduce_kernel,
        out_shape=jax.ShapeDtypeStruct((3 * TILE, width), f32),
        in_specs=[pl.BlockSpec(memory_space=pl.ANY)],
        out_specs=pl.BlockSpec(memory_space=pltpu.VMEM),
        scratch_shapes=[
            pltpu.VMEM((2, 2, piece_len, width), f32),
            pltpu.VMEM((2, 2, piece_len, width), f32),
            pltpu.VMEM((piece_len, width), f32),
            pltpu.VMEM((piece_len, width), f32),
            pltpu.VMEM((4, 3, TILE, width), f32),
            dma((2, 2)),
            dma((2, 2)),
            dma((2, 2)),
            dma((N_CHUNK,)),
            dma((N_CHUNK,)),
            dma((N_CHUNK,)),
            dma((N_CHUNK,)),
            dma((2, piece_len // TILE)),
            dma((4, 3)),
        ],
        compiler_params=pltpu.CompilerParams(collective_id=3, has_side_effects=True, vmem_limit_bytes=VMEM_LIMIT),
        cost_estimate=pl.CostEstimate(flops=20_000_000_000, bytes_accessed=30_000_000, transcendentals=0),
        name="reduce_kv",
    )(part)


def dot_nt(lhs, rhs):
    return lax.dot_general(lhs, rhs, (((1,), (1,)), ((), ())), preferred_element_type=jnp.float32)


def dot_nn(lhs, rhs):
    return lax.dot_general(lhs, rhs, (((1,), (0,)), ((), ())), preferred_element_type=jnp.float32)


def causal(shape, k_start, q_start):
    k_pos = k_start + lax.broadcasted_iota(jnp.int32, shape, 0)
    q_pos = q_start + lax.broadcasted_iota(jnp.int32, shape, 1) % TILE
    return k_pos <= q_pos


def forward_kernel(info, q_ref, k_ref, v_ref, o_ref, lse_ref, q_all, acc, run_max, run_sum):
    tile = pl.program_id(0)
    q_start = info[1, tile]
    last = q_start // KBLK
    head_dim = k_ref.shape[2]
    n_heads = q_ref.shape[1] // head_dim
    for head in range(n_heads):
        q_all[pl.ds(head * TILE, TILE), :] = q_ref[:, pl.ds(head * head_dim, head_dim)]
    acc[...] = jnp.zeros_like(acc)
    run_max[...] = jnp.full_like(run_max, -jnp.inf)
    run_sum[...] = jnp.zeros_like(run_sum)

    def block(k_idx, masked):
        k_start = pl.multiple_of(k_idx * KBLK, KBLK)
        key_blk = k_ref[0, pl.ds(k_start, KBLK), :]
        val_blk = v_ref[0, pl.ds(k_start, KBLK), :].T
        for chunk in range(n_heads * TILE // CHUNK):
            rows = pl.ds(chunk * CHUNK, CHUNK)
            scores = dot_nt(key_blk, q_all[rows, :])
            if masked:
                scores = jnp.where(causal(scores.shape, k_start, q_start), scores, -jnp.inf)
            old_max = run_max[:, rows]
            new_max = jnp.maximum(old_max, jnp.max(scores, axis=0, keepdims=True))
            rescale = jnp.exp(old_max - new_max)
            weights = jnp.exp(scores - new_max)
            run_max[:, rows] = new_max
            run_sum[:, rows] = run_sum[:, rows] * rescale + jnp.sum(weights, axis=0, keepdims=True)
            acc[:, rows] = acc[:, rows] * rescale + dot_nn(val_blk, weights.astype(jnp.bfloat16))

    def body(k_idx, carry):
        block(k_idx, False)
        return carry

    lax.fori_loop(0, last, body, 0)
    block(last, True)
    lse_ref[0] = run_max[...] + jnp.log(run_sum[...])
    inv_sum = 1.0 / run_sum[...]
    for head in range(n_heads):
        rows = pl.ds(head * TILE, TILE)
        o_ref[:, pl.ds(head * head_dim, head_dim)] = (acc[:, rows] * inv_sum[:, head * TILE : (head + 1) * TILE]).T.astype(jnp.bfloat16)


def backward_kernel(info, q_ref, do_ref, lse_ref, delta_ref, k_ref, v_ref, dq_ref, dkv_ref, q_all, do_all, dq_acc):
    tile = pl.program_id(0)
    q_start = info[1, tile]
    last = q_start // KBLK
    head_dim = k_ref.shape[2]
    n_heads = q_ref.shape[1] // head_dim
    for head in range(n_heads):
        q_all[pl.ds(head * TILE, TILE), :] = q_ref[:, pl.ds(head * head_dim, head_dim)]
        do_all[pl.ds(head * TILE, TILE), :] = do_ref[:, pl.ds(head * head_dim, head_dim)]
    dq_acc[...] = jnp.zeros_like(dq_acc)

    @pl.when(info[3, tile] == 1)
    def _():
        dkv_ref[...] = jnp.zeros_like(dkv_ref)

    def block(k_idx, masked):
        k_start = pl.multiple_of(k_idx * KBLK, KBLK)
        keys = pl.ds(k_start, KBLK)
        key_blk = k_ref[0, keys, :]
        val_blk = v_ref[0, keys, :]
        keyt_blk = key_blk.T
        dk_part = jnp.zeros((KBLK, head_dim), jnp.float32)
        dv_part = jnp.zeros((KBLK, head_dim), jnp.float32)
        for chunk in range(n_heads * TILE // CHUNK):
            rows = pl.ds(chunk * CHUNK, CHUNK)
            q_rows, do_rows = q_all[rows, :], do_all[rows, :]
            probs = jnp.exp(dot_nt(key_blk, q_rows) - lse_ref[0, :, rows])
            if masked:
                probs = jnp.where(causal(probs.shape, k_start, q_start), probs, 0.0)
            d_score = (probs * (dot_nt(val_blk, do_rows) - delta_ref[0, :, rows])).astype(jnp.bfloat16)
            dv_part += dot_nn(probs.astype(jnp.bfloat16), do_rows)
            dk_part += dot_nn(d_score, q_rows)
            dq_acc[:, rows] += dot_nn(keyt_blk, d_score)
        dkv_ref[0, keys, pl.ds(0, head_dim)] += dk_part
        dkv_ref[0, keys, pl.ds(head_dim, head_dim)] += dv_part

    def body(k_idx, carry):
        block(k_idx, False)
        return carry

    lax.fori_loop(0, last, body, 0)
    block(last, True)
    for head in range(n_heads):
        dq_ref[:, pl.ds(head * head_dim, head_dim)] = dq_acc[:, pl.ds(head * TILE, TILE)].T


def attention_forward(info, queries, kv_all):
    n_rows, width = queries.shape
    n_keys, head_dim = kv_all.shape[1], kv_all.shape[2] // 2
    all_rows = width // head_dim * TILE
    return pl.pallas_call(
        forward_kernel,
        out_shape=[
            jax.ShapeDtypeStruct((n_rows, width), jnp.bfloat16),
            jax.ShapeDtypeStruct((n_rows // TILE, 1, all_rows), jnp.float32),
        ],
        grid_spec=pltpu.PrefetchScalarGridSpec(
            num_scalar_prefetch=1,
            grid=(n_rows // TILE,),
            in_specs=[
                pl.BlockSpec((TILE, width), lambda i, info: (i, 0)),
                pl.BlockSpec((1, n_keys, head_dim), lambda i, info: (info[0, i], 0, 0)),
                pl.BlockSpec((1, n_keys, head_dim), lambda i, info: (info[0, i], 0, 1)),
            ],
            out_specs=[
                pl.BlockSpec((TILE, width), lambda i, info: (i, 0)),
                pl.BlockSpec((1, 1, all_rows), lambda i, info: (i, 0, 0)),
            ],
            scratch_shapes=[
                pltpu.VMEM((all_rows, head_dim), jnp.bfloat16),
                pltpu.VMEM((head_dim, all_rows), jnp.float32),
                pltpu.VMEM((1, all_rows), jnp.float32),
                pltpu.VMEM((1, all_rows), jnp.float32),
            ],
        ),
        compiler_params=pltpu.CompilerParams(vmem_limit_bytes=VMEM_LIMIT),
        cost_estimate=pl.CostEstimate(flops=8_000_000_000, bytes_accessed=10_000_000, transcendentals=6_000_000),
        name="attention_forward",
    )(info, queries, kv_all, kv_all)


def attention_backward(info, queries, d_out, row_lse, row_delta, kv_all):
    n_rows, width = queries.shape
    n_keys, head_dim = kv_all.shape[1], kv_all.shape[2] // 2
    all_rows = width // head_dim * TILE
    return pl.pallas_call(
        backward_kernel,
        out_shape=[
            jax.ShapeDtypeStruct((n_rows, width), jnp.float32),
            jax.ShapeDtypeStruct((2, n_keys, 2 * head_dim), jnp.float32),
        ],
        grid_spec=pltpu.PrefetchScalarGridSpec(
            num_scalar_prefetch=1,
            grid=(n_rows // TILE,),
            in_specs=[
                pl.BlockSpec((TILE, width), lambda i, info: (i, 0)),
                pl.BlockSpec((TILE, width), lambda i, info: (i, 0)),
                pl.BlockSpec((1, 1, all_rows), lambda i, info: (i, 0, 0)),
                pl.BlockSpec((1, 1, all_rows), lambda i, info: (i, 0, 0)),
                pl.BlockSpec((1, n_keys, head_dim), lambda i, info: (info[0, i], 0, 0)),
                pl.BlockSpec((1, n_keys, head_dim), lambda i, info: (info[0, i], 0, 1)),
            ],
            out_specs=[
                pl.BlockSpec((TILE, width), lambda i, info: (i, 0)),
                pl.BlockSpec((1, n_keys, 2 * head_dim), lambda i, info: (info[2, i], 0, 0)),
            ],
            scratch_shapes=[
                pltpu.VMEM((all_rows, head_dim), jnp.bfloat16),
                pltpu.VMEM((all_rows, head_dim), jnp.bfloat16),
                pltpu.VMEM((head_dim, all_rows), jnp.float32),
            ],
        ),
        compiler_params=pltpu.CompilerParams(vmem_limit_bytes=VMEM_LIMIT),
        cost_estimate=pl.CostEstimate(flops=20_000_000_000, bytes_accessed=20_000_000, transcendentals=6_000_000),
        name="attention_backward",
    )(info, queries, d_out, row_lse, row_delta, kv_all, kv_all)


def solution(mesh):
    tp_size, cp_size = mesh.shape["tp"], mesh.shape["cp"]

    def local_program(hidden, grad_out, w_query, w_key, w_value, w_out):
        n_batch, block_len, width = hidden.shape
        head_dim = w_key.shape[1]
        n_heads = tp_size
        q_scale = head_dim ** -0.5
        tp_idx, cp_idx = lax.axis_index("tp"), lax.axis_index("cp")
        n_tokens = n_batch * block_len
        n_rows = n_tokens // tp_size
        row0 = tp_idx * n_rows
        hid_flat = hidden.reshape(n_tokens, width)
        grad_flat = grad_out.reshape(n_tokens, width)
        hid_own = lax.dynamic_slice_in_dim(hid_flat, row0, n_rows, 0)
        grad_own = lax.dynamic_slice_in_dim(grad_flat, row0, n_rows, 0)

        cos_piece, sin_piece = rope_tables(cp_idx * block_len + jnp.arange(block_len), head_dim)
        key_pre = jnp.einsum("bsd,de->bse", hidden, w_key, preferred_element_type=jnp.float32)
        key_loc = rotate(key_pre, cos_piece, sin_piece).astype(jnp.bfloat16)
        val_loc = jnp.einsum("bsd,de->bse", hidden, w_value, preferred_element_type=jnp.float32).astype(jnp.bfloat16)
        kv_loc = jnp.concatenate([key_loc, val_loc], axis=-1)
        kv_all = lax.all_gather(kv_loc, "cp", axis=1, tiled=True)

        wq_all, wo_all = gather_tp([w_query.reshape(width, head_dim), w_out.reshape(head_dim, width)], 0, shared=True)
        wq_all = wq_all.reshape(n_heads, width, head_dim)

        own_pos = cp_idx * block_len + (row0 + jnp.arange(n_rows)) % block_len
        cos_own, sin_own = rope_tables(own_pos, head_dim)
        cos_q, sin_q = cos_own[:, None, :], sin_own[:, None, :]
        q_pre = jnp.einsum("rd,nde->rne", hid_own, wq_all, preferred_element_type=jnp.float32)
        queries = (rotate(q_pre, cos_q, sin_q) * q_scale).astype(jnp.bfloat16).reshape(n_rows, n_heads * head_dim)
        d_out = jnp.einsum("rd,fd->rf", grad_own, wo_all, preferred_element_type=jnp.float32).astype(jnp.bfloat16)

        n_tiles = n_rows // TILE
        tile_ids = tp_idx * n_tiles + jnp.arange(n_tiles)
        per_batch = block_len // TILE
        tile_batch = tile_ids // per_batch
        tile_slot = (tile_batch != tile_batch[1]).astype(tile_ids.dtype)
        fresh = jnp.concatenate([jnp.ones((1,), tile_slot.dtype), jnp.abs(tile_slot[1:] - tile_slot[:-1])])
        info = jnp.stack([tile_batch, cp_idx * block_len + tile_ids % per_batch * TILE, tile_slot, fresh]).astype(jnp.int32)

        attn_own, row_lse = attention_forward(info, queries, kv_all)
        attn_all = lax.all_gather(attn_own, "tp", axis=0, tiled=True)
        row_delta = jnp.einsum("rne,rne->rn", d_out.reshape(n_rows, n_heads, head_dim), attn_own.reshape(n_rows, n_heads, head_dim), preferred_element_type=jnp.float32)
        row_delta = row_delta.reshape(n_tiles, TILE, n_heads).transpose(0, 2, 1).reshape(n_tiles, 1, n_heads * TILE)
        dq_own, dkv_slots = attention_backward(info, queries, d_out, row_lse, row_delta, kv_all)
        dq_pre = (unrotate(dq_own.reshape(n_rows, n_heads, head_dim), cos_q, sin_q) * q_scale).astype(jnp.bfloat16)

        dkv_own = reduce_kv(dkv_slots)
        dk_own = unrotate(dkv_own[:, :head_dim], cos_own, sin_own).astype(jnp.bfloat16)
        dv_own = dkv_own[:, head_dim:].astype(jnp.bfloat16)

        (dkv_piece,) = gather_tp([jnp.concatenate([dk_own, dv_own], axis=-1)], 1)
        attn_head = lax.dynamic_slice_in_dim(attn_all, tp_idx * head_dim, head_dim, 1)
        d_w_out = jnp.einsum("rf,rd->fd", attn_head, grad_flat, preferred_element_type=jnp.float32)
        d_w_kv = jnp.einsum("rd,rf->df", hid_flat, dkv_piece, preferred_element_type=jnp.float32)
        dq_all, d_w_out, d_w_kv = gather_tp([dq_pre.reshape(n_rows, n_heads * head_dim)], 2, sums=[d_w_out, d_w_kv])
        dq_head = lax.dynamic_slice_in_dim(dq_all, tp_idx * head_dim, head_dim, 1)
        d_w_query = lax.psum(jnp.einsum("rd,rf->df", hid_flat, dq_head, preferred_element_type=jnp.float32), "cp")
        attn_out = jnp.einsum("rf,fd->rd", attn_all, wo_all, preferred_element_type=jnp.float32).astype(jnp.bfloat16)
        d_hidden = jnp.einsum("rne,nde->rd", dq_all.reshape(n_tokens, n_heads, head_dim), wq_all, preferred_element_type=jnp.float32)
        d_hidden += jnp.einsum("rf,df->rd", dkv_piece, jnp.concatenate([w_key, w_value], axis=1), preferred_element_type=jnp.float32)
        return (
            attn_out.reshape(hidden.shape),
            d_hidden.astype(jnp.bfloat16).reshape(hidden.shape),
            d_w_query[:, None, :],
            d_w_kv[:, :head_dim],
            d_w_kv[:, head_dim:],
            d_w_out[None],
        )

    row_spec = P(None, "cp", None)
    return jax.shard_map(local_program, mesh=mesh, in_specs=(row_spec, row_spec, P(None, "tp", None), P(), P(), P("tp", None, None)), out_specs=(row_spec, row_spec, P(None, "tp", None), P(), P(), P("tp", None, None)), check_vma=False)
```

```python
import functools

import jax
import jax.numpy as jnp
from jax import lax
from jax.experimental import pallas as pl
from jax.experimental.pallas import tpu as pltpu
from jax.sharding import PartitionSpec as P

ROPE_BASE = 10000.0
MESH = pl.DeviceIdType.MESH
TILE = 128
KBLK = 512
CHUNK = 512
VMEM_LIMIT = 60 * 1024 * 1024


def rope_tables(positions, head_dim):
    half_dim = head_dim // 2
    inv_freq = 1.0 / jnp.power(ROPE_BASE, jnp.arange(half_dim, dtype=jnp.float32) * (2.0 / head_dim))
    angles = positions.astype(jnp.float32)[:, None] * inv_freq[None, :]
    return jnp.cos(angles), jnp.sin(angles)


def rotate(rot_in, cos_tab, sin_tab):
    half_dim = rot_in.shape[-1] // 2
    low_half = rot_in[..., :half_dim]
    high_half = rot_in[..., half_dim:]
    return jnp.concatenate([low_half * cos_tab - high_half * sin_tab, high_half * cos_tab + low_half * sin_tab], axis=-1)


def unrotate(rot_in, cos_tab, sin_tab):
    return rotate(rot_in, cos_tab, -sin_tab)


def gather_kernel(n_arrays, shared, n_sums, *refs):
    n_in = n_arrays + n_sums
    ins, sum_ins = refs[:n_arrays], refs[n_arrays:n_in]
    outs, sum_outs = refs[n_in : n_in + n_arrays], refs[n_in + n_arrays : 2 * n_in]
    near, far = refs[2 * n_in : 2 * n_in + n_sums], refs[2 * n_in + n_sums : 2 * n_in + 2 * n_sums]
    send_sems, recv_sems, local_sems = refs[2 * n_in + 2 * n_sums : 2 * n_in + 2 * n_sums + 3]
    sum_sems = refs[2 * n_in + 2 * n_sums + 3 :]
    me, core = lax.axis_index("tp"), lax.axis_index("cp") % 2
    z_idx, y_idx = me // 2, me % 2
    right, left, part = me + 2, me - 2, z_idx * 2 + 1 - y_idx
    has_right, has_left = z_idx < 3, z_idx > 0
    sibling = lax.axis_index("cp") + 1 - 2 * core

    barrier = pltpu.get_barrier_semaphore()

    def greet(device):
        pl.semaphore_signal(barrier, inc=1, device_id=device, device_id_type=MESH)
        return None

    greet({"tp": part})
    across = (lax.axis_index("cp") + 2) % 4
    extra = 1
    if shared or n_sums:
        greet({"cp": sibling})
        extra += 1
    if n_sums:
        greet({"cp": across})
        extra += 1

    @pl.when(has_right)
    def _():
        greet({"tp": right})

    @pl.when(has_left)
    def _():
        greet({"tp": left})

    ends = jnp.where(has_right, 1, 0) + jnp.where(has_left, 1, 0)
    pl.semaphore_wait(barrier, ends + extra)

    def geometry(i):
        whole = outs[i].shape[0] // 8
        rows = whole // 2 if shared else whole
        return whole, rows, (core * rows if shared else 0)

    def segment(rows, seg):
        a_len = (rows // 12 + 8) // 16 * 16
        b_len = rows // 2 - a_len
        return {
            "A0": (0, a_len),
            "A1": (rows - a_len, a_len),
            "B": (a_len, 2 * b_len),
            "B0": (a_len, b_len),
            "B1": (rows // 2, b_len),
            "H0": (0, rows // 2),
            "H1": (rows // 2, rows // 2),
        }[seg]

    names = ["yA0", "yA1", "yB"] + [f"{kind}{s}{h}" for kind in ("R", "L", "yR", "yL", "pR", "pL") for s in range(3) for h in range(2)]
    index = {name: k for k, name in enumerate(names)}

    def describe(name, receiving):
        if name[:2] in ("yA", "yB") and len(name) <= 3:
            return name[1:], z_idx, (1 - y_idx if receiving else y_idx), part, None, not receiving
        kind, s, h = name[:-2], int(name[-2]), name[-1]
        sign = -1 if "R" in kind else 1
        if kind in ("yR", "yL"):
            z_src = z_idx + sign * (1 + s)
            ok = z_src >= 0 if sign < 0 else z_src < 4
            return "B" + h, z_src, (1 - y_idx if receiving else y_idx), part, ok, False
        seg = ("H" if len(kind) == 1 else "A") + h
        y_src = y_idx if len(kind) == 1 else 1 - y_idx
        if receiving:
            z_src = z_idx + sign * (1 + s)
            ok = z_src >= 0 if sign < 0 else z_src < 4
        else:
            z_src = z_idx + sign * s
            ok = (z_src >= 0) & has_right if sign < 0 else (z_src < 4) & has_left
        return seg, z_src, y_src, (right if sign < 0 else left), ok, len(kind) == 1 and s == 0 and not receiving

    def each(name, receiving, act):
        seg, z_src, y_src, target, ok, own = describe(name, receiving)

        def run():
            for i in range(n_arrays):
                whole, rows, offset = geometry(i)
                first, count = segment(rows, seg)
                span = pl.ds(pl.multiple_of((z_src * 2 + y_src) * whole + offset + first, 16), count)
                own_span = pl.ds(pl.multiple_of(offset + first, 16), count)
                act(
                    pltpu.make_async_remote_copy(
                        src_ref=ins[i].at[own_span] if own else outs[i].at[span],
                        dst_ref=outs[i].at[span],
                        send_sem=send_sems.at[i, index[name]],
                        recv_sem=recv_sems.at[i, index[name]],
                        device_id={"tp": target},
                        device_id_type=MESH,
                    )
                )

        if ok is None:
            run()
        else:
            pl.when(ok)(run)

    def start(*which):
        for name in which:
            each(name, False, lambda copy: copy.start())

    def arrive(*which):
        for name in which:
            each(name, True, lambda copy: copy.wait_recv())

    def half_of(i, which):
        half = sum_ins[i].shape[0] // 2
        return pl.ds(pl.multiple_of(which * half, 8), half)

    def sum_copy(i, stage):
        src = (sum_ins[i].at[half_of(i, 1 - core)], near[i], far[i])[stage]
        dst = (near[i], far[i], sum_outs[i].at[half_of(i, core)])[stage]
        return pltpu.make_async_remote_copy(
            src_ref=src,
            dst_ref=dst,
            send_sem=sum_sems[0].at[i, stage],
            recv_sem=sum_sems[1].at[i, stage],
            device_id={"cp": across if stage == 1 else sibling},
            device_id_type=MESH,
        )

    def sum_last(i):
        span = half_of(i, 1 - core)
        return pltpu.make_async_remote_copy(
            src_ref=far[i],
            dst_ref=sum_outs[i].at[span],
            send_sem=sum_sems[0].at[i, 2],
            recv_sem=sum_sems[1].at[i, 2],
            device_id={"cp": sibling},
            device_id_type=MESH,
        )

    def sum_store(i):
        return pltpu.make_async_copy(far[i], sum_outs[i].at[half_of(i, core)], sum_sems[2].at[i])

    def add_rows(dst, src, first):
        step = 32

        def body(n, carry):
            rows = pl.ds(pl.multiple_of(n * step, step), step)
            src_rows = pl.ds(pl.multiple_of(first + n * step, step), step)
            dst[rows, :] += src[src_rows, :]
            return carry

        lax.fori_loop(0, dst.shape[0] // step, body, 0)

    def sums_begin():
        for i in range(n_sums):
            sum_copy(i, 0).start()

    def sums_middle():
        for i in range(n_sums):
            sum_copy(i, 0).wait_recv()
            add_rows(near[i], sum_ins[i], core * (sum_ins[i].shape[0] // 2))
            sum_copy(i, 1).start()

    def sums_finish():
        for i in range(n_sums):
            sum_copy(i, 1).wait_recv()
            add_rows(far[i], near[i], 0)
            sum_copy(i, 2).start()
            sum_store(i).start()

    def sums_drain():
        for i in range(n_sums):
            sum_last(i).wait_recv()
            sum_store(i).wait()
            for stage in range(3):
                sum_copy(i, stage).wait_send()

    start("yA0", "R00", "L00", "yA1", "R01", "L01", "yB")
    sums_begin()
    own = []
    for i in range(n_arrays):
        whole, rows, offset = geometry(i)
        span = pl.ds(pl.multiple_of(me * whole + offset, 16), rows)
        own_span = pl.ds(pl.multiple_of(offset, 16), rows) if shared else pl.ds(0, rows)
        own.append(pltpu.make_async_copy(ins[i].at[own_span], outs[i].at[span], local_sems.at[i]))
        own[-1].start()
    for s in range(3):
        for h in "01":
            for side in "RL":
                arrive(f"{side}{s}{h}")
                if s < 2:
                    start(f"{side}{s + 1}{h}")
                start(f"y{side}{s}{h}")
        if s == 0:
            arrive("yA0", "yA1")
            sums_middle()
        for side in "RL":
            for h in "01":
                if s > 0:
                    arrive(f"p{side}{s - 1}{h}")
                start(f"p{side}{s}{h}")
    sums_finish()
    arrive("pR20", "pR21", "pL20", "pL21", "yB")
    for side in "RL":
        for s in range(3):
            for h in "01":
                arrive(f"y{side}{s}{h}")
    for name in names:
        each(name, False, lambda copy: copy.wait_send())
    for copy in own:
        copy.wait()
    sums_drain()
    if shared:
        last = len(names)
        swaps = []
        for i in range(n_arrays):
            whole, rows, offset = geometry(i)
            for block in range(8):
                span = pl.ds(pl.multiple_of(block * whole + offset, 16), rows)
                swaps.append(
                    pltpu.make_async_remote_copy(
                        src_ref=outs[i].at[span],
                        dst_ref=outs[i].at[span],
                        send_sem=send_sems.at[i, last + block],
                        recv_sem=recv_sems.at[i, last + block],
                        device_id={"cp": sibling},
                        device_id_type=MESH,
                    )
                )
                swaps[-1].start()
        for copy in swaps:
            copy.wait_send()
        for i in range(n_arrays):
            whole, rows, offset = geometry(i)
            for block in range(8):
                span = pl.ds(pl.multiple_of(block * whole + rows - offset, 16), rows)
                pltpu.make_async_remote_copy(
                    src_ref=outs[i].at[span],
                    dst_ref=outs[i].at[span],
                    send_sem=send_sems.at[i, last + block],
                    recv_sem=recv_sems.at[i, last + block],
                    device_id={"cp": sibling},
                    device_id_type=MESH,
                ).wait_recv()


def gather_tp(arrays, collective_id, shared=False, sums=()):
    n_arrays, n_sums = len(arrays), len(sums)
    n_steps = 3 + 6 * 6 + (8 if shared else 0)
    sent = sum(a.size * a.dtype.itemsize for a in arrays)
    dma = pltpu.SemaphoreType.DMA
    halves = [pltpu.VMEM((a.shape[0] // 2, a.shape[1]), a.dtype) for a in sums]
    return pl.pallas_call(
        functools.partial(gather_kernel, n_arrays, shared, n_sums),
        out_shape=[jax.ShapeDtypeStruct((8 * a.shape[0], a.shape[1]), a.dtype) for a in arrays]
        + [jax.ShapeDtypeStruct(a.shape, a.dtype) for a in sums],
        in_specs=[pl.BlockSpec(memory_space=pltpu.VMEM)] * (n_arrays + n_sums),
        out_specs=[pl.BlockSpec(memory_space=pl.ANY)] * (n_arrays + n_sums),
        scratch_shapes=halves
        + halves
        + [dma((n_arrays, n_steps)), dma((n_arrays, n_steps)), dma((n_arrays,))]
        + ([dma((n_sums, 3)), dma((n_sums, 3)), dma((n_sums,))] if n_sums else []),
        compiler_params=pltpu.CompilerParams(collective_id=collective_id, has_side_effects=True, vmem_limit_bytes=VMEM_LIMIT),
        cost_estimate=pl.CostEstimate(flops=sent * 20000, bytes_accessed=9 * sent, transcendentals=0),
        name=f"gather_tp_{collective_id}",
    )(*arrays, *sums)


N_CHUNK = 4


def reduce_kernel(part, out, acc, sib, side, back, tiles, ld_sem, s1_send, s1_recv, y_send, y_recv, x_send, x_recv, t_send, t_recv):
    me, cp_idx = lax.axis_index("tp"), lax.axis_index("cp")
    core, x_idx = cp_idx % 2, cp_idx // 2
    piece_len = acc.shape[2]
    chunk = piece_len // N_CHUNK
    partner = me + 1 - 2 * (me % 2)
    sibling = cp_idx + 1 - 2 * core
    across = cp_idx + 2 - 4 * x_idx
    straddles = (me == 2) | (me == 5)
    merges = (me == 3) | (me == 4)
    main_batch = (3 * me + 1) // 8

    def base(batch):
        return 5 * batch // 2

    def limit(batch):
        return (5 * batch + 7) // 2

    barrier = pltpu.get_barrier_semaphore()
    for step in range(1, 8):
        pl.semaphore_signal(barrier, inc=1, device_id={"tp": (me + step) % 8}, device_id_type=MESH)
    pl.semaphore_signal(barrier, inc=1, device_id={"cp": sibling}, device_id_type=MESH)
    pl.semaphore_signal(barrier, inc=1, device_id={"cp": across}, device_id_type=MESH)
    pl.semaphore_wait(barrier, 9)

    def piece(idx):
        return pl.ds(pl.multiple_of(idx * piece_len, piece_len), piece_len)

    def load(slot, k):
        return pltpu.make_async_copy(part.at[slot, piece(2 * k + core)], acc.at[slot, k], ld_sem.at[slot, k])

    def to_sibling(slot, k):
        return pltpu.make_async_remote_copy(
            src_ref=part.at[slot, piece(2 * k + 1 - core)],
            dst_ref=sib.at[slot, k],
            send_sem=s1_send.at[slot, k],
            recv_sem=s1_recv.at[slot, k],
            device_id={"cp": sibling},
            device_id_type=MESH,
        )

    def rows_of(c):
        return pl.ds(c * chunk, chunk)

    def to_partner(c):
        return pltpu.make_async_remote_copy(
            src_ref=acc.at[1, 0, rows_of(c)],
            dst_ref=side.at[rows_of(c)],
            send_sem=y_send.at[c],
            recv_sem=y_recv.at[c],
            device_id={"tp": partner},
            device_id_type=MESH,
        )

    def across_x(c):
        return pltpu.make_async_remote_copy(
            src_ref=acc.at[0, 0, rows_of(c)],
            dst_ref=back.at[rows_of(c)],
            send_sem=x_send.at[c],
            recv_sem=x_recv.at[c],
            device_id={"cp": across},
            device_id_type=MESH,
        )

    def to_owner(slot, i):
        batch = 1 if slot else main_batch
        tile = 8 * batch + i
        return pltpu.make_async_remote_copy(
            src_ref=acc.at[slot, x_idx, pl.ds(i * TILE, TILE)],
            dst_ref=tiles.at[me - base(batch), tile % 3],
            send_sem=t_send.at[slot, i],
            recv_sem=t_recv.at[me - base(batch), tile % 3],
            device_id={"tp": tile // 3},
            device_id_type=MESH,
        )

    def not_mine(slot, i):
        return (8 * (1 if slot else main_batch) + i) // 3 != me

    def for_slots(act):
        for k in range(2):
            for slot in range(2):
                conds = []
                if k == 1:
                    conds.append(x_idx == 1)
                if slot == 1:
                    conds.append(straddles)
                run = functools.partial(act, slot, k)
                if conds:
                    pl.when(functools.reduce(jnp.logical_and, conds))(run)
                else:
                    run()

    def begin(slot, k):
        to_sibling(slot, k).start()
        load(slot, k).start()

    def join(slot, k):
        load(slot, k).wait()
        to_sibling(slot, k).wait_recv()
        for c in range(N_CHUNK):
            acc[slot, k, rows_of(c)] += sib[slot, k, rows_of(c)]
        if slot == 1 and k == 0:
            @pl.when(x_idx == 1)
            def _():
                for c in range(N_CHUNK):
                    to_partner(c).start()

        if slot == 1:
            @pl.when(x_idx == k)
            def _():
                for i in range(piece_len // TILE):
                    pl.when(not_mine(1, i))(to_owner(1, i).start)

    for_slots(begin)
    for_slots(join)

    def finish(k, c):
        if k == 0:
            @pl.when(merges & (x_idx == 1))
            def _():
                to_partner(c).wait_recv()
                acc[0, 0, rows_of(c)] += side[rows_of(c)]

            @pl.when(x_idx == 1)
            def _():
                across_x(c).start()

            @pl.when(x_idx == 0)
            def _():
                across_x(c).wait_recv()
                acc[0, 0, rows_of(c)] += back[rows_of(c)]

        @pl.when(x_idx == k)
        def _():
            for i in range(c * chunk // TILE, (c + 1) * chunk // TILE):
                pl.when(not_mine(0, i))(to_owner(0, i).start)

    for c in range(N_CHUNK):
        finish(0, c)

    @pl.when(x_idx == 1)
    def _():
        for c in range(N_CHUNK):
            finish(1, c)

    for local in range(3):
        tile = 3 * me + local
        batch = tile // 8
        rows = pl.ds(local * TILE, TILE)
        first_rank = base(batch)
        out[rows, :] = jnp.zeros((TILE, out.shape[1]), jnp.float32)

        @pl.when(batch == main_batch)
        def _():
            out[rows, :] += acc[0, x_idx, pl.ds(pl.multiple_of((tile - 8 * batch) * TILE, TILE), TILE)]

        @pl.when(batch != main_batch)
        def _():
            out[rows, :] += acc[1, x_idx, pl.ds(pl.multiple_of((tile - 8 * batch) * TILE, TILE), TILE)]

        for rank in range(4):
            @pl.when((first_rank + rank < limit(batch)) & (first_rank + rank != me))
            def _():
                pltpu.make_async_remote_copy(
                    src_ref=tiles.at[rank, local],
                    dst_ref=tiles.at[rank, local],
                    send_sem=t_send.at[0, 0],
                    recv_sem=t_recv.at[rank, local],
                    device_id={"tp": partner},
                    device_id_type=MESH,
                ).wait_recv()
                out[rows, :] += tiles[rank, local]

    def drain(slot, k):
        to_sibling(slot, k).wait_send()
        if slot == 1 and k == 0:
            @pl.when(x_idx == 1)
            def _():
                for c in range(N_CHUNK):
                    to_partner(c).wait_send()

        if slot == 1:
            @pl.when(x_idx == k)
            def _():
                for i in range(piece_len // TILE):
                    pl.when(not_mine(1, i))(to_owner(1, i).wait_send)

    for_slots(drain)

    @pl.when(x_idx == 1)
    def _():
        for c in range(N_CHUNK):
            across_x(c).wait_send()

    for i in range(piece_len // TILE):
        pl.when(not_mine(0, i))(to_owner(0, i).wait_send)


def reduce_kv(part):
    n_slots, n_keys, width = part.shape
    piece_len = n_keys // 4
    dma = pltpu.SemaphoreType.DMA
    f32 = jnp.float32
    return pl.pallas_call(
        reduce_kernel,
        out_shape=jax.ShapeDtypeStruct((3 * TILE, width), f32),
        in_specs=[pl.BlockSpec(memory_space=pl.ANY)],
        out_specs=pl.BlockSpec(memory_space=pltpu.VMEM),
        scratch_shapes=[
            pltpu.VMEM((2, 2, piece_len, width), f32),
            pltpu.VMEM((2, 2, piece_len, width), f32),
            pltpu.VMEM((piece_len, width), f32),
            pltpu.VMEM((piece_len, width), f32),
            pltpu.VMEM((4, 3, TILE, width), f32),
            dma((2, 2)),
            dma((2, 2)),
            dma((2, 2)),
            dma((N_CHUNK,)),
            dma((N_CHUNK,)),
            dma((N_CHUNK,)),
            dma((N_CHUNK,)),
            dma((2, piece_len // TILE)),
            dma((4, 3)),
        ],
        compiler_params=pltpu.CompilerParams(collective_id=3, has_side_effects=True, vmem_limit_bytes=VMEM_LIMIT),
        cost_estimate=pl.CostEstimate(flops=20_000_000_000, bytes_accessed=30_000_000, transcendentals=0),
        name="reduce_kv",
    )(part)


def dot_nt(lhs, rhs):
    return lax.dot_general(lhs, rhs, (((1,), (1,)), ((), ())), preferred_element_type=jnp.float32)


def dot_nn(lhs, rhs):
    return lax.dot_general(lhs, rhs, (((1,), (0,)), ((), ())), preferred_element_type=jnp.float32)


def causal(shape, k_start, q_start):
    k_pos = k_start + lax.broadcasted_iota(jnp.int32, shape, 0)
    q_pos = q_start + lax.broadcasted_iota(jnp.int32, shape, 1) % TILE
    return k_pos <= q_pos


def forward_kernel(info, q_ref, k_ref, v_ref, o_ref, lse_ref, q_all, acc, run_max, run_sum):
    tile = pl.program_id(0)
    q_start = info[1, tile]
    last = q_start // KBLK
    head_dim = k_ref.shape[2]
    n_heads = q_ref.shape[1] // head_dim
    for head in range(n_heads):
        q_all[pl.ds(head * TILE, TILE), :] = q_ref[:, pl.ds(head * head_dim, head_dim)]
    acc[...] = jnp.zeros_like(acc)
    run_max[...] = jnp.full_like(run_max, -jnp.inf)
    run_sum[...] = jnp.zeros_like(run_sum)

    def block(k_idx, masked):
        k_start = pl.multiple_of(k_idx * KBLK, KBLK)
        key_blk = k_ref[0, pl.ds(k_start, KBLK), :]
        val_blk = v_ref[0, pl.ds(k_start, KBLK), :].T
        for chunk in range(n_heads * TILE // CHUNK):
            rows = pl.ds(chunk * CHUNK, CHUNK)
            scores = dot_nt(key_blk, q_all[rows, :])
            if masked:
                scores = jnp.where(causal(scores.shape, k_start, q_start), scores, -jnp.inf)
            old_max = run_max[:, rows]
            new_max = jnp.maximum(old_max, jnp.max(scores, axis=0, keepdims=True))
            rescale = jnp.exp(old_max - new_max)
            weights = jnp.exp(scores - new_max)
            run_max[:, rows] = new_max
            run_sum[:, rows] = run_sum[:, rows] * rescale + jnp.sum(weights, axis=0, keepdims=True)
            acc[:, rows] = acc[:, rows] * rescale + dot_nn(val_blk, weights.astype(jnp.bfloat16))

    def body(k_idx, carry):
        block(k_idx, False)
        return carry

    lax.fori_loop(0, last, body, 0)
    block(last, True)
    lse_ref[0] = run_max[...] + jnp.log(run_sum[...])
    inv_sum = 1.0 / run_sum[...]
    for head in range(n_heads):
        rows = pl.ds(head * TILE, TILE)
        o_ref[:, pl.ds(head * head_dim, head_dim)] = (acc[:, rows] * inv_sum[:, head * TILE : (head + 1) * TILE]).T.astype(jnp.bfloat16)


def backward_kernel(info, q_ref, do_ref, lse_ref, delta_ref, k_ref, v_ref, dq_ref, dkv_ref, q_all, do_all, dq_acc):
    tile = pl.program_id(0)
    q_start = info[1, tile]
    last = q_start // KBLK
    head_dim = k_ref.shape[2]
    n_heads = q_ref.shape[1] // head_dim
    for head in range(n_heads):
        q_all[pl.ds(head * TILE, TILE), :] = q_ref[:, pl.ds(head * head_dim, head_dim)]
        do_all[pl.ds(head * TILE, TILE), :] = do_ref[:, pl.ds(head * head_dim, head_dim)]
    dq_acc[...] = jnp.zeros_like(dq_acc)

    @pl.when(info[3, tile] == 1)
    def _():
        dkv_ref[...] = jnp.zeros_like(dkv_ref)

    def block(k_idx, masked):
        k_start = pl.multiple_of(k_idx * KBLK, KBLK)
        keys = pl.ds(k_start, KBLK)
        key_blk = k_ref[0, keys, :]
        val_blk = v_ref[0, keys, :]
        keyt_blk = key_blk.T
        dk_part = jnp.zeros((KBLK, head_dim), jnp.float32)
        dv_part = jnp.zeros((KBLK, head_dim), jnp.float32)
        for chunk in range(n_heads * TILE // CHUNK):
            rows = pl.ds(chunk * CHUNK, CHUNK)
            q_rows, do_rows = q_all[rows, :], do_all[rows, :]
            probs = jnp.exp(dot_nt(key_blk, q_rows) - lse_ref[0, :, rows])
            if masked:
                probs = jnp.where(causal(probs.shape, k_start, q_start), probs, 0.0)
            d_score = (probs * (dot_nt(val_blk, do_rows) - delta_ref[0, :, rows])).astype(jnp.bfloat16)
            dv_part += dot_nn(probs.astype(jnp.bfloat16), do_rows)
            dk_part += dot_nn(d_score, q_rows)
            dq_acc[:, rows] += dot_nn(keyt_blk, d_score)
        dkv_ref[0, keys, pl.ds(0, head_dim)] += dk_part
        dkv_ref[0, keys, pl.ds(head_dim, head_dim)] += dv_part

    def body(k_idx, carry):
        block(k_idx, False)
        return carry

    lax.fori_loop(0, last, body, 0)
    block(last, True)
    for head in range(n_heads):
        dq_ref[:, pl.ds(head * head_dim, head_dim)] = dq_acc[:, pl.ds(head * TILE, TILE)].T


def attention_forward(info, queries, kv_all):
    n_rows, width = queries.shape
    n_keys, head_dim = kv_all.shape[1], kv_all.shape[2] // 2
    all_rows = width // head_dim * TILE
    return pl.pallas_call(
        forward_kernel,
        out_shape=[
            jax.ShapeDtypeStruct((n_rows, width), jnp.bfloat16),
            jax.ShapeDtypeStruct((n_rows // TILE, 1, all_rows), jnp.float32),
        ],
        grid_spec=pltpu.PrefetchScalarGridSpec(
            num_scalar_prefetch=1,
            grid=(n_rows // TILE,),
            in_specs=[
                pl.BlockSpec((TILE, width), lambda i, info: (i, 0)),
                pl.BlockSpec((1, n_keys, head_dim), lambda i, info: (info[0, i], 0, 0)),
                pl.BlockSpec((1, n_keys, head_dim), lambda i, info: (info[0, i], 0, 1)),
            ],
            out_specs=[
                pl.BlockSpec((TILE, width), lambda i, info: (i, 0)),
                pl.BlockSpec((1, 1, all_rows), lambda i, info: (i, 0, 0)),
            ],
            scratch_shapes=[
                pltpu.VMEM((all_rows, head_dim), jnp.bfloat16),
                pltpu.VMEM((head_dim, all_rows), jnp.float32),
                pltpu.VMEM((1, all_rows), jnp.float32),
                pltpu.VMEM((1, all_rows), jnp.float32),
            ],
        ),
        compiler_params=pltpu.CompilerParams(vmem_limit_bytes=VMEM_LIMIT),
        cost_estimate=pl.CostEstimate(flops=8_000_000_000, bytes_accessed=10_000_000, transcendentals=6_000_000),
        name="attention_forward",
    )(info, queries, kv_all, kv_all)


def attention_backward(info, queries, d_out, row_lse, row_delta, kv_all):
    n_rows, width = queries.shape
    n_keys, head_dim = kv_all.shape[1], kv_all.shape[2] // 2
    all_rows = width // head_dim * TILE
    return pl.pallas_call(
        backward_kernel,
        out_shape=[
            jax.ShapeDtypeStruct((n_rows, width), jnp.float32),
            jax.ShapeDtypeStruct((2, n_keys, 2 * head_dim), jnp.float32),
        ],
        grid_spec=pltpu.PrefetchScalarGridSpec(
            num_scalar_prefetch=1,
            grid=(n_rows // TILE,),
            in_specs=[
                pl.BlockSpec((TILE, width), lambda i, info: (i, 0)),
                pl.BlockSpec((TILE, width), lambda i, info: (i, 0)),
                pl.BlockSpec((1, 1, all_rows), lambda i, info: (i, 0, 0)),
                pl.BlockSpec((1, 1, all_rows), lambda i, info: (i, 0, 0)),
                pl.BlockSpec((1, n_keys, head_dim), lambda i, info: (info[0, i], 0, 0)),
                pl.BlockSpec((1, n_keys, head_dim), lambda i, info: (info[0, i], 0, 1)),
            ],
            out_specs=[
                pl.BlockSpec((TILE, width), lambda i, info: (i, 0)),
                pl.BlockSpec((1, n_keys, 2 * head_dim), lambda i, info: (info[2, i], 0, 0)),
            ],
            scratch_shapes=[
                pltpu.VMEM((all_rows, head_dim), jnp.bfloat16),
                pltpu.VMEM((all_rows, head_dim), jnp.bfloat16),
                pltpu.VMEM((head_dim, all_rows), jnp.float32),
            ],
        ),
        compiler_params=pltpu.CompilerParams(vmem_limit_bytes=VMEM_LIMIT),
        cost_estimate=pl.CostEstimate(flops=20_000_000_000, bytes_accessed=20_000_000, transcendentals=6_000_000),
        name="attention_backward",
    )(info, queries, d_out, row_lse, row_delta, kv_all, kv_all)


def solution(mesh):
    tp_size, cp_size = mesh.shape["tp"], mesh.shape["cp"]

    def local_program(hidden, grad_out, w_query, w_key, w_value, w_out):
        n_batch, block_len, width = hidden.shape
        head_dim = w_key.shape[1]
        n_heads = tp_size
        q_scale = head_dim ** -0.5
        tp_idx, cp_idx = lax.axis_index("tp"), lax.axis_index("cp")
        n_tokens = n_batch * block_len
        n_rows = n_tokens // tp_size
        row0 = tp_idx * n_rows
        hid_flat = hidden.reshape(n_tokens, width)
        grad_flat = grad_out.reshape(n_tokens, width)
        hid_own = lax.dynamic_slice_in_dim(hid_flat, row0, n_rows, 0)
        grad_own = lax.dynamic_slice_in_dim(grad_flat, row0, n_rows, 0)

        cos_piece, sin_piece = rope_tables(cp_idx * block_len + jnp.arange(block_len), head_dim)
        key_pre = jnp.einsum("bsd,de->bse", hidden, w_key, preferred_element_type=jnp.float32)
        key_loc = rotate(key_pre, cos_piece, sin_piece).astype(jnp.bfloat16)
        val_loc = jnp.einsum("bsd,de->bse", hidden, w_value, preferred_element_type=jnp.float32).astype(jnp.bfloat16)
        kv_loc = jnp.concatenate([key_loc, val_loc], axis=-1)
        kv_all = lax.all_gather(kv_loc, "cp", axis=1, tiled=True)

        wq_all, wo_all = gather_tp([w_query.reshape(width, head_dim), w_out.reshape(head_dim, width)], 0, shared=True)
        wq_all = wq_all.reshape(n_heads, width, head_dim)

        own_pos = cp_idx * block_len + (row0 + jnp.arange(n_rows)) % block_len
        cos_own, sin_own = rope_tables(own_pos, head_dim)
        cos_q, sin_q = cos_own[:, None, :], sin_own[:, None, :]
        q_pre = jnp.einsum("rd,nde->rne", hid_own, wq_all, preferred_element_type=jnp.float32)
        queries = (rotate(q_pre, cos_q, sin_q) * q_scale).astype(jnp.bfloat16).reshape(n_rows, n_heads * head_dim)
        d_out = jnp.einsum("rd,fd->rf", grad_own, wo_all, preferred_element_type=jnp.float32).astype(jnp.bfloat16)

        n_tiles = n_rows // TILE
        tile_ids = tp_idx * n_tiles + jnp.arange(n_tiles)
        per_batch = block_len // TILE
        tile_batch = tile_ids // per_batch
        tile_slot = (tile_batch != tile_batch[1]).astype(tile_ids.dtype)
        fresh = jnp.concatenate([jnp.ones((1,), tile_slot.dtype), jnp.abs(tile_slot[1:] - tile_slot[:-1])])
        info = jnp.stack([tile_batch, cp_idx * block_len + tile_ids % per_batch * TILE, tile_slot, fresh]).astype(jnp.int32)

        attn_own, row_lse = attention_forward(info, queries, kv_all)
        attn_all = lax.all_gather(attn_own, "tp", axis=0, tiled=True)
        row_delta = jnp.einsum("rne,rne->rn", d_out.reshape(n_rows, n_heads, head_dim), attn_own.reshape(n_rows, n_heads, head_dim), preferred_element_type=jnp.float32)
        row_delta = row_delta.reshape(n_tiles, TILE, n_heads).transpose(0, 2, 1).reshape(n_tiles, 1, n_heads * TILE)
        dq_own, dkv_slots = attention_backward(info, queries, d_out, row_lse, row_delta, kv_all)
        dq_pre = (unrotate(dq_own.reshape(n_rows, n_heads, head_dim), cos_q, sin_q) * q_scale).astype(jnp.bfloat16)

        dkv_own = reduce_kv(dkv_slots)
        dk_own = unrotate(dkv_own[:, :head_dim], cos_own, sin_own).astype(jnp.bfloat16)
        dv_own = dkv_own[:, head_dim:].astype(jnp.bfloat16)

        (dkv_piece,) = gather_tp([jnp.concatenate([dk_own, dv_own], axis=-1)], 1)
        attn_head = lax.dynamic_slice_in_dim(attn_all, tp_idx * head_dim, head_dim, 1)
        d_w_out = jnp.einsum("rf,rd->fd", attn_head, grad_flat, preferred_element_type=jnp.float32)
        d_w_kv = jnp.einsum("rd,rf->df", hid_flat, dkv_piece, preferred_element_type=jnp.float32)
        dq_all, d_w_out, d_w_kv = gather_tp([dq_pre.reshape(n_rows, n_heads * head_dim)], 2, sums=[d_w_out, d_w_kv])
        dq_head = lax.dynamic_slice_in_dim(dq_all, tp_idx * head_dim, head_dim, 1)
        d_w_query = lax.psum(jnp.einsum("rd,rf->df", hid_flat, dq_head, preferred_element_type=jnp.float32), "cp")
        attn_out = jnp.einsum("rf,fd->rd", attn_all, wo_all, preferred_element_type=jnp.float32).astype(jnp.bfloat16)
        d_hidden = jnp.einsum("rne,nde->rd", dq_all.reshape(n_tokens, n_heads, head_dim), wq_all, preferred_element_type=jnp.float32)
        d_hidden += jnp.einsum("rf,df->rd", dkv_piece, jnp.concatenate([w_key, w_value], axis=1), preferred_element_type=jnp.float32)
        return (
            attn_out.reshape(hidden.shape),
            d_hidden.astype(jnp.bfloat16).reshape(hidden.shape),
            d_w_query[:, None, :],
            d_w_kv[:, :head_dim],
            d_w_kv[:, head_dim:],
            d_w_out[None],
        )

    row_spec = P(None, "cp", None)
    return jax.shard_map(local_program, mesh=mesh, in_specs=(row_spec, row_spec, P(None, "tp", None), P(), P(), P("tp", None, None)), out_specs=(row_spec, row_spec, P(None, "tp", None), P(), P(), P("tp", None, None)), check_vma=False)
```
